32 devices in a mesh: seq: 8 (over y, x, core), head: 4 (over z).
Axes of the slice: x: 2, y: 2, z: 4, core: 2. Of those that a mesh axis runs over, the one named last changes fastest.
Arguments:
- positions: int32 [4096], P('seq'), may hold values from 65535 to 73725, as said below
- queries: bfloat16 [4096, 32, 128], P('seq', 'head'), may hold values from -16 to 16
- keys: bfloat16 [4096, 16, 128], P('seq', 'head'), may hold values from -16 to 16
- values: bfloat16 [4096, 16, 128], P('seq', 'head'), may hold values from -6 to 6
- out_weight: bfloat16 [4096, 5376], P('head', 'seq'), may hold values from -0.125 to 0.125
- post_gain: float32 [5376], P('head'), may hold values from 0.25 to 1.75
- residual: bfloat16 [4096, 5376], P('seq', 'head'), may hold values from -6 to 6
Outputs:
- layer_out: bfloat16 [4096, 5376], P('seq', 'head')
The draws below stay inside these ranges and needn't reach their ends.
Inputs may be any that keep to these rules, and one draw needn't show every extreme that they name: `positions`: strictly rising, by 1 or 2 from one token to the next; the last token's position is the most.
All inputs are finite; a program needn't handle non-finite values.
Results may differ from the reference program's by a relative error of at most 0.015.
Values may be sent and summed in bfloat16 or wider, within the bound.
A program may use at most 128 MiB of HBM per device.

```python
import jax
import jax.numpy as jnp
from jax import lax

D = 5376
QUERY_HEADS = 32
KEY_VALUE_HEADS = 16
HEAD_SIZE = 128
VISIBLE_SPAN = 1024
SLAB_TOKENS = 4096
N_HEAD = 4


def draw_positions(key, part):
    spacing = jax.random.randint(jax.random.fold_in(key, 22), (SLAB_TOKENS,), 1, 3).astype(jnp.int32)
    after = jnp.cumsum(spacing[::-1])[::-1] - spacing
    last_position = 65535 + 2 * SLAB_TOKENS - 2
    return (last_position - after).astype(jnp.int32)


def draw_keys(key, part):
    drawn_output = jnp.clip(jax.random.normal(jax.random.fold_in(key, 11), (SLAB_TOKENS, KEY_VALUE_HEADS, HEAD_SIZE), jnp.float32), -16.0, 16.0)
    return drawn_output.astype(jnp.bfloat16)


def draw_queries(key, part):
    drawn_output = jnp.clip(jax.random.normal(jax.random.fold_in(key, 12), (SLAB_TOKENS, QUERY_HEADS, HEAD_SIZE), jnp.float32), -16.0, 16.0)
    return drawn_output.astype(jnp.bfloat16)


def spiked(values, rng, source, target, shards_of, factor):
    def block_of(position):
        return (jnp.arange(values.shape[position]) // (values.shape[position] // shards_of)).reshape((-1,) + (1,) * (values.ndim - 1 - position))

    near = jax.random.permutation(rng, shards_of)[block_of(target)]
    other_side = (block_of(target) + shards_of // 2) % shards_of
    return jnp.where((block_of(source) == near) | (block_of(source) == other_side), factor * values, values)


def shard_levels(key, shape, shards, least, largest):
    gain, own = 1.0, jax.random.fold_in(key, 6)
    for dim, parts in shards:
        steps = jnp.exp(jax.random.uniform(jax.random.fold_in(own, dim), (parts,), jnp.float32, least / len(shards), largest / len(shards)))
        gain = gain * jnp.repeat(steps, shape[dim] // parts).reshape([-1 if axis == dim else 1 for axis in range(len(shape))])
    return gain


def gaussian(own_key, extent, scale, bound, pieces=(), kind=jnp.bfloat16):
    array = scale * jax.random.normal(own_key, extent, jnp.float32)
    if pieces:
        array = array * shard_levels(own_key, extent, pieces, -0.22, 0.18)
    return jnp.clip(array, -bound, bound).astype(kind)


def heavy_noise(stream_key, shape, deviation, most, cuts, heavy, kind=jnp.bfloat16):
    entries = deviation * jax.random.normal(stream_key, shape, jnp.float32)
    if cuts:
        entries = entries * shard_levels(stream_key, shape, cuts, -0.22, 0.18)
    return jnp.clip(spiked(entries, jax.random.fold_in(stream_key, 3), *heavy), -most, most).astype(kind)


def setup_inputs(seed: int = 0) -> dict:
    key_of = jax.random.split(jax.random.key(seed), 8)
    positions = draw_positions(jax.random.fold_in(key_of[7], 71), 0)
    queries = draw_queries(jax.random.fold_in(key_of[7], 71), 0)
    keys = draw_keys(jax.random.fold_in(key_of[7], 71), 0)
    values = gaussian(key_of[3], (SLAB_TOKENS, KEY_VALUE_HEADS, HEAD_SIZE), 1.0, 6.0, ((0, 8), (1, 4)))
    out_weight = heavy_noise(key_of[4], (QUERY_HEADS * HEAD_SIZE, D), (QUERY_HEADS * HEAD_SIZE) ** -0.5, 0.125, ((0, 4), (1, 8)), (0, 1, 8, 2.0))
    post_gain = jnp.clip(1.0 + 0.15 * jax.random.normal(key_of[5], (D,), jnp.float32), 0.25, 1.75)
    residual = gaussian(key_of[6], (SLAB_TOKENS, D), 1.0, 6.0, ((0, 8), (1, 4)))
    return dict(positions=positions, queries=queries, keys=keys, values=values, out_weight=out_weight, post_gain=post_gain, residual=residual)


EPS = 1e-06
SCALE = 168.0 ** (-0.5)

def rotate(x, positions):
    half = x.shape[-1] // 2
    inverse = 10000.0 ** (-2.0 * jnp.arange(half, dtype=jnp.float32) / x.shape[-1])
    angle = positions.astype(jnp.float32)[:, None] * inverse[None, :]
    cosine = jnp.concatenate([jnp.cos(angle), jnp.cos(angle)], -1)[:, None, :]
    sine = jnp.concatenate([jnp.sin(angle), jnp.sin(angle)], -1)[:, None, :]
    source = x.astype(jnp.float32)
    turned = jnp.concatenate([-source[..., half:], source[..., :half]], -1)
    return (source * cosine + turned * sine).astype(jnp.bfloat16)

def reference(positions, queries, keys, values, out_weight, post_gain, residual):
    q_rot = rotate(queries, positions)
    k_rot = rotate(keys, positions)
    query_groups = QUERY_HEADS // KEY_VALUE_HEADS
    padding_length = jnp.zeros((VISIBLE_SPAN, KEY_VALUE_HEADS, HEAD_SIZE), jnp.bfloat16)
    key_pad = jnp.concatenate([padding_length, k_rot], 0)
    value_pad = jnp.concatenate([padding_length, values], 0)
    block_length = min(512, SLAB_TOKENS)

    def attend(number):
        first = (number * block_length).astype(jnp.int32)
        query_tile_rows = lax.dynamic_slice_in_dim(q_rot, first, block_length, 0).astype(jnp.float32)
        query_tile_rows = query_tile_rows.reshape(block_length, KEY_VALUE_HEADS, query_groups, HEAD_SIZE)
        key_block = lax.dynamic_slice_in_dim(key_pad, first, block_length + VISIBLE_SPAN, 0).astype(jnp.float32)
        value_block = lax.dynamic_slice_in_dim(value_pad, first, block_length + VISIBLE_SPAN, 0).astype(jnp.float32)
        scores = jnp.einsum('qhgd,khd->hgqk', query_tile_rows, key_block) * SCALE
        query_index = jnp.arange(block_length, dtype=jnp.int32)
        key_index = jnp.arange(block_length + VISIBLE_SPAN, dtype=jnp.int32)
        gap = VISIBLE_SPAN + query_index[:, None] - key_index[None, :]
        token_of_key = first - VISIBLE_SPAN + key_index
        allowed = (gap >= 0) & (gap < VISIBLE_SPAN) & (token_of_key[None, :] >= 0)
        scores = jnp.where(allowed, scores, -1e+30)
        top = lax.optimization_barrier(jnp.max(scores, axis=-1, keepdims=True))
        weights = jnp.exp(scores - top)
        probs = (weights / lax.optimization_barrier(jnp.sum(weights, axis=-1, keepdims=True))).astype(jnp.bfloat16)
        context = jnp.einsum('hgqk,khd->qhgd', probs.astype(jnp.float32), value_block)
        return context.astype(jnp.bfloat16).reshape(block_length, QUERY_HEADS * HEAD_SIZE)
    context = lax.map(attend, jnp.arange(SLAB_TOKENS // block_length, dtype=jnp.int32)).reshape(SLAB_TOKENS, QUERY_HEADS * HEAD_SIZE)
    width = QUERY_HEADS * HEAD_SIZE // N_HEAD
    attended = jnp.zeros((SLAB_TOKENS, D), jnp.float32)
    for group in range(N_HEAD):
        partial_value = jnp.dot(context[:, group * width:(group + 1) * width], out_weight[group * width:(group + 1) * width], preferred_element_type=jnp.float32)
        attended = attended + partial_value.astype(jnp.bfloat16).astype(jnp.float32)
    mean_square = lax.optimization_barrier(jnp.mean(attended * attended, axis=1, keepdims=True))
    result = residual.astype(jnp.float32) + post_gain[None, :] * attended * lax.rsqrt(mean_square + EPS)
    return result.astype(jnp.bfloat16)
```

```python
import functools

import jax
import jax.numpy as jnp
from jax import lax
from jax.experimental import pallas as pl
from jax.experimental.pallas import tpu as pltpu
from jax.sharding import PartitionSpec as P

D = 5376
QUERY_HEADS = 32
KEY_VALUE_HEADS = 16
VISIBLE_SPAN = 1024


EPS = 1e-06
SCALE = 168.0 ** (-0.5)
LOG2E = 1.4426950408889634
MASKED = -1e30
TILE = 256
LANES = 128
MESH = pl.DeviceIdType.MESH
LAUNCH = (
    "Z0", "Z1", "Z2", "Z3", "Z4", "Z5", "Z6", "H0", "H1", "H2", "H3",
)
PLAN = (
    "T6", "T0", "T1", "T2", "T3", "T4", "T5", "C0", "A0", "A1", "C1", "A2",
    "A3", "C2", "C3", "R10", "R11", "R12", "R13", "X0", "Y0", "D0", "S0", "P002",
    "R20", "R21", "P022", "R22", "R23", "X1", "Y1", "D1", "S1", "P102", "R30", "P122",
    "R31", "R32", "R33", "X2", "Y2", "D2", "S2", "P202", "P222", "X3", "Y3", "D3",
    "S3", "P302", "P32", "P33",
)
DIRECT = (0, 1, 2, 3, )


def passed_along(value, axis, steps):
    count = lax.axis_size(axis)
    initial, last = (max(0, -steps), min(count, count - steps))
    return lax.ppermute(value, axis, [(source, source + steps) for source in range(initial, last)])


def rotate(x, positions):
    half = x.shape[-1] // 2
    inverse = 10000.0 ** (-2.0 * jnp.arange(half, dtype=jnp.float32) / x.shape[-1])
    angle = positions.astype(jnp.float32)[:, None] * inverse[None, :]
    cosine = jnp.concatenate([jnp.cos(angle), jnp.cos(angle)], -1)[:, None, :]
    sine = jnp.concatenate([jnp.sin(angle), jnp.sin(angle)], -1)[:, None, :]
    source = x.astype(jnp.float32)
    turned = jnp.concatenate([-source[..., half:], source[..., :half]], -1)
    return (source * cosine + turned * sine).astype(jnp.bfloat16)


def layer_kernel(
    n_seq, n_head, kv_heads, groups, reach,
    q_ref, k_ref, v_ref, w_ref, gain_ref, res_ref, out_ref,
    k_ext, v_ext, stage, w_all, ctx, acc, squares,
    halo_send, halo_recv, pass_send, a_send, a_recv, own_sem, c_send, c_recv,
    unit_send, forward_send, relay_send, unit_recv,
    up_send, down_send, ctx_recv, sq_send, sq_recv,
):
    me = lax.axis_index("seq")
    z = lax.axis_index("head")
    rows = k_ref.shape[1]
    size = k_ref.shape[2]
    feats = w_ref.shape[0]
    sub = n_seq // n_head
    span = reach * rows
    core = lax.rem(me, 2)
    chip = me // 2
    even = core == 0
    sibling = me + 1 - 2 * core
    across = me + 2 - 4 * lax.rem(chip, 2)
    along = me + 4 - 8 * (chip // 2)
    corner = across + along - me
    pair = groups * size

    def remote(src, dst, send, recv, device):
        return pltpu.make_async_remote_copy(
            src_ref=src, dst_ref=dst, send_sem=send, recv_sem=recv,
            device_id=device, device_id_type=MESH,
        )

    def order(s):
        low = z < n_head // 2
        near = jnp.where(low, z, n_head - 1 - z)
        at = near if s == 0 else (1 - near if s == 1 else s)
        return jnp.where(low, at, n_head - 1 - at)

    def halo(dist, g, kv, target):
        at = pl.ds(span - dist * rows, rows)
        if kv == 0:
            src, dst = k_ref.at[g], k_ext.at[g, at, :]
        else:
            src, dst = v_ref.at[g], v_ext.at[g, :, at]
        return remote(src, dst, halo_send.at[dist - 1, g, kv], halo_recv.at[dist - 1, g, kv], (target, z))

    def passed_on(g, kv):
        near, far = pl.ds(span - rows, rows), pl.ds(span - 2 * rows, rows)
        if kv == 0:
            src, dst = k_ext.at[g, near, :], k_ext.at[g, far, :]
        else:
            src, dst = v_ext.at[g, :, near], v_ext.at[g, :, far]
        return remote(src, dst, pass_send.at[g, kv], halo_recv.at[1, g, kv], (me + 1, z))

    def start_halo(g):
        @pl.when(me + 1 < n_seq)
        def _():
            halo(1, g, 0, me + 1).start()
            halo(1, g, 1, me + 1).start()

        @pl.when(jnp.logical_and(even, me + 2 < n_seq))
        def _():
            halo(2, g, 0, me + 2).start()
            halo(2, g, 1, me + 2).start()

    def columns(target):
        return w_ref.at[:, pl.ds(pl.multiple_of(target * LANES, LANES), LANES)]

    def piece(source, target, direct):
        dst = w_all.at[target, z, lax.rem(source, sub)] if direct else stage.at[source]
        return remote(columns(target), dst, a_send.at[target], a_recv.at[source], (target, z))

    def scatter(target):
        @pl.when(me // sub == z)
        def _():
            piece(me, target, True).start()

        @pl.when(me // sub != z)
        def _():
            piece(me, target, False).start()

    def own_copy():
        return pltpu.make_async_copy(columns(me), w_all.at[me, z, lax.rem(me, sub)], own_sem)

    def own_climb():
        return remote(
            columns(me), w_all.at[me, z, lax.rem(me, sub)],
            c_send.at[me], c_recv.at[z, lax.rem(me, sub)], (me, me // sub),
        )

    def climb(source):
        return remote(
            stage.at[source], w_all.at[me, z, lax.rem(source, sub)],
            c_send.at[source], c_recv.at[z, lax.rem(source, sub)], (me, source // sub),
        )

    def take_piece(source):
        piece(source, me, False).wait_recv()

        @pl.when(source // sub != z)
        def _():
            climb(source).start()

    others = (across, along, across + 1 - 2 * core, along + 1 - 2 * core, corner, corner + 1 - 2 * core, sibling)

    def unit(owner, r, send, target):
        return remote(w_all.at[owner, r], w_all.at[owner, r], send, unit_recv.at[owner, r], (target, z))

    def send_unit(s):
        r = order(s)
        if s == 0:
            @pl.when(me // sub == z)
            def _():
                own_copy().wait()

        else:
            for j in range(sub):
                remote(stage.at[0], w_all.at[me, r, j], c_send.at[0], c_recv.at[r, j], (me, r)).wait_recv()
        unit(me, r, unit_send.at[0, s], across).start()
        unit(me, r, unit_send.at[1, s], along).start()
        if s in DIRECT:
            unit(me, r, forward_send.at[s], corner).start()
        unit(me, r, relay_send.at[0, s], sibling).start()

    def take_across(s):
        r = order(s)
        unit(across, r, unit_send.at[0, s], me).wait_recv()

        @pl.when(jnp.logical_and(even, s not in DIRECT))
        def _():
            unit(across, r, forward_send.at[s], along).start()

        unit(across, r, relay_send.at[1, s], sibling).start()

    def take_along(s):
        r = order(s)
        unit(along, r, unit_send.at[0, s], me).wait_recv()

        @pl.when(jnp.logical_and(jnp.logical_not(even), s not in DIRECT))
        def _():
            unit(along, r, forward_send.at[s], across).start()

        unit(along, r, relay_send.at[2, s], sibling).start()

    def take_corner(s):
        r = order(s)
        unit(corner, r, unit_send.at[0, s], me).wait_recv()
        unit(corner, r, relay_send.at[3, s], sibling).start()

    def take_relayed(s):
        r = order(s)
        for owner in (me, across, along, corner):
            unit(owner + 1 - 2 * core, r, unit_send.at[0, s], me).wait_recv()

    def chunk(r, g):
        return ctx.at[r, pl.ds(g * pair, pair), :]

    def ctx_up(r, g):
        return remote(chunk(r, g), chunk(r, g), up_send.at[r, g], ctx_recv.at[r, g], (me, z + 1))

    def ctx_down(r, g):
        return remote(chunk(r, g), chunk(r, g), down_send.at[r, g], ctx_recv.at[r, g], (me, z - 1))

    inner = jnp.logical_and(z >= 1, z + 1 < n_head)

    def arrive(s, g):
        r = order(s)

        @pl.when(inner)
        def _():
            ctx_up(r, g).wait_recv()

        @pl.when(jnp.logical_and(inner, r < z))
        def _():
            ctx_up(r, g).start()

        @pl.when(jnp.logical_and(inner, r > z))
        def _():
            ctx_down(r, g).start()

    blocks = span // TILE + 1

    def attend(g):
        for dist in range(1, reach + 1):
            @pl.when(me >= dist)
            def _():
                halo(dist, g, 0, me).wait_recv()
                halo(dist, g, 1, me).wait_recv()
                if dist == 1:
                    @pl.when(even)
                    def _():
                        passed_on(g, 0).start()
                        passed_on(g, 1).start()

        @pl.loop(0, rows // TILE)
        def _(t):
            first = pl.multiple_of(t * TILE, TILE)
            q = jnp.concatenate([q_ref[g * groups + i, pl.ds(first, TILE), :] for i in range(groups)], 0)
            row = lax.broadcasted_iota(jnp.int32, (TILE, groups * TILE), 0)
            col = lax.rem(lax.broadcasted_iota(jnp.int32, (TILE, groups * TILE), 1), TILE)
            scores = []
            top = None
            for b in range(blocks):
                s = lax.dot_general(
                    k_ext[g, pl.ds(first + b * TILE, TILE), :], q,
                    (((1,), (1,)), ((), ())), preferred_element_type=jnp.float32,
                )
                valid = me * rows + first + b * TILE - span >= 0
                if b == 0:
                    s = jnp.where(jnp.logical_and(row > col, valid), s, MASKED)
                elif b == blocks - 1:
                    s = jnp.where(row <= col, s, MASKED)
                else:
                    s = jnp.where(valid, s, MASKED)
                scores.append(s)
                high = jnp.max(s, axis=0, keepdims=True)
                top = high if top is None else jnp.maximum(top, high)
            shift = top * (SCALE * LOG2E)
            total = None
            mixed = None
            for b in range(blocks):
                w = jnp.exp2(scores[b] * (SCALE * LOG2E) - shift)
                part_sum = jnp.sum(w, axis=0, keepdims=True)
                total = part_sum if total is None else total + part_sum
                o = jnp.dot(
                    v_ext[g, :, pl.ds(pl.multiple_of(first + b * TILE, TILE), TILE)], w.astype(jnp.bfloat16),
                    preferred_element_type=jnp.float32,
                )
                mixed = o if mixed is None else mixed + o
            result = (mixed / total).astype(jnp.bfloat16)
            for i in range(groups):
                ctx[z, pl.ds((g * groups + i) * size, size), pl.ds(first, TILE)] = result[:, i * TILE : (i + 1) * TILE]

        @pl.when(z + 1 < n_head)
        def _():
            ctx_up(z, g).start()

        @pl.when(z >= 1)
        def _():
            ctx_down(z, g).start()

    tile = next(t for t in range(256, 0, -16) if feats % t == 0)

    def project(s, g, n=1):
        r = order(s)
        if s > 0:
            @pl.when(jnp.logical_not(inner))
            def _():
                for i in range(n):
                    ctx_up(r, g + i).wait_recv()

        block = ctx[r, pl.ds(g * pair, n * pair), :]
        for j in range(sub):
            @pl.loop(0, feats // tile)
            def _(t):
                at = pl.ds(pl.multiple_of(t * tile, tile), tile)
                w = jnp.concatenate([w_all[g * groups + i, r, j, at, :] for i in range(n * groups)], 1)
                got = jnp.dot(w, block, preferred_element_type=jnp.float32)
                if s == 0 and g == 0:
                    acc[j, at, :] = got
                else:
                    acc[j, at, :] += got

    barrier = pltpu.get_barrier_semaphore()
    for d in range(1, n_seq):
        pl.semaphore_signal(barrier, inc=1, device_id=(lax.rem(me + d, n_seq), z), device_id_type=MESH)
    for d in range(1, n_head):
        pl.semaphore_signal(barrier, inc=1, device_id=(me, lax.rem(z + d, n_head)), device_id_type=MESH)
    pl.semaphore_wait(barrier, n_seq + n_head - 2)

    @pl.when(me // sub == z)
    def _():
        own_copy().start()

    @pl.when(me // sub != z)
    def _():
        own_climb().start()

    for word in LAUNCH:
        if word[0] == "H":
            start_halo(int(word[1]))
        else:
            scatter(others[int(word[1])])

    for dist in range(1, reach + 1):
        @pl.when(me < dist)
        def _():
            at = pl.ds(span - dist * rows, rows)
            k_ext[:, at, :] = jnp.zeros((kv_heads, rows, size), jnp.bfloat16)
            v_ext[:, :, at] = jnp.zeros((kv_heads, size, rows), jnp.bfloat16)
    k_ext[:, pl.ds(span, rows), :] = k_ref[...]
    v_ext[:, :, pl.ds(span, rows)] = v_ref[...]

    def take(n):
        take_piece(others[n])

    steps = {"T": take, "A": attend, "C": send_unit, "X": take_across, "Y": take_along, "D": take_corner,
             "S": take_relayed, "R": arrive, "P": project}
    for word in PLAN:
        steps[word[0]](*[int(c) for c in word[1:]])

    mine = jnp.zeros((8, rows), jnp.float32)
    for j in range(sub):
        value = acc[j]
        mine = mine + jnp.sum((value * value).reshape(feats // 8, 8, rows), axis=0)
    squares[0] = mine

    def sq(d, target):
        return remote(squares.at[0], squares.at[d], sq_send.at[d - 1], sq_recv.at[d - 1], (me, target))

    for d in range(1, n_head):
        sq(d, lax.rem(z + d, n_head)).start()
    for d in range(1, n_head):
        sq(d, z).wait_recv()
    whole = jnp.sum(jnp.sum(squares[...], axis=0), axis=0, keepdims=True)
    inverse = lax.rsqrt(whole / (n_head * sub * feats) + EPS)
    for j in range(sub):
        at = pl.ds(j * feats, feats)
        out_ref[at, :] = (
            res_ref[at, :].astype(jnp.float32) + gain_ref[at, :] * (acc[j] * inverse)
        ).astype(jnp.bfloat16)

    for d in range(1, n_head):
        sq(d, z).wait_send()
    for g in range(kv_heads):
        for dist in range(1, reach + 1):
            leaves = me + dist < n_seq
            if dist == 2:
                leaves = jnp.logical_and(even, leaves)

            @pl.when(leaves)
            def _():
                halo(dist, g, 0, me).wait_send()
                halo(dist, g, 1, me).wait_send()

        @pl.when(jnp.logical_and(even, me >= 1))
        def _():
            passed_on(g, 0).wait_send()
            passed_on(g, 1).wait_send()
    for target in others:
        piece(me, target, False).wait_send()
        source = target

        @pl.when(source // sub != z)
        def _():
            climb(source).wait_send()

    @pl.when(me // sub != z)
    def _():
        own_climb().wait_send()
    for s in range(n_head):
        for way in range(2):
            unit(me, s, unit_send.at[way, s], me).wait_send()
        unit(me, s, forward_send.at[s], me).wait_send()
        for way in range(4):
            unit(me, s, relay_send.at[way, s], me).wait_send()
    for g in range(kv_heads):
        for r in range(n_head):
            @pl.when(jnp.logical_and(r <= z, z + 1 < n_head))
            def _():
                ctx_up(r, g).wait_send()

            @pl.when(jnp.logical_and(r >= z, z >= 1))
            def _():
                ctx_down(r, g).wait_send()


def fits(rows, heads_rows, kv_heads, groups, feats, n_seq, n_head):
    return (
        n_seq == 8
        and n_head in (2, 4)
        and groups == 2
        and heads_rows == n_seq * LANES
        and rows % TILE == 0
        and VISIBLE_SPAN == 2 * rows
        and kv_heads * groups == n_seq
        and feats % 16 == 0
    )


def fused(positions, queries, keys, values, out_weight, post_gain, residual):
    n_seq, n_head = lax.axis_size("seq"), lax.axis_size("head")
    rows, kv_heads, size = keys.shape
    groups = queries.shape[1] // kv_heads
    feats = out_weight.shape[1]
    width = residual.shape[1]
    sub = n_seq // n_head
    reach = VISIBLE_SPAN // rows
    q = rotate(queries, positions).transpose(1, 0, 2)
    k = rotate(keys, positions).transpose(1, 0, 2)
    v = values.transpose(1, 2, 0)
    bf16, f32 = jnp.bfloat16, jnp.float32
    dma = pltpu.SemaphoreType.DMA
    spec = pl.BlockSpec(memory_space=pltpu.VMEM)
    out = pl.pallas_call(
        functools.partial(layer_kernel, n_seq, n_head, kv_heads, groups, reach),
        out_shape=jax.ShapeDtypeStruct((width, rows), bf16),
        in_specs=[spec] * 6,
        out_specs=spec,
        scratch_shapes=[
            pltpu.VMEM((kv_heads, (reach + 1) * rows, size), bf16),
            pltpu.VMEM((kv_heads, size, (reach + 1) * rows), bf16),
            pltpu.VMEM((n_seq, feats, LANES), bf16),
            pltpu.VMEM((n_seq, n_head, sub, feats, LANES), bf16),
            pltpu.VMEM((n_head, kv_heads * groups * size, rows), bf16),
            pltpu.VMEM((sub, feats, rows), f32),
            pltpu.VMEM((n_head, 8, rows), f32),
            dma((reach, kv_heads, 2)), dma((reach, kv_heads, 2)), dma((kv_heads, 2)),
            dma((n_seq,)), dma((n_seq,)), dma, dma((n_seq,)), dma((n_head, sub)),
            dma((2, n_head)), dma((n_head,)), dma((4, n_head)), dma((n_seq, n_head)),
            dma((n_head, kv_heads)), dma((n_head, kv_heads)), dma((n_head, kv_heads)),
            dma((n_head,)), dma((n_head,)),
        ],
        compiler_params=pltpu.CompilerParams(has_side_effects=True, collective_id=0, vmem_limit_bytes=60 * 1024 * 1024),
    )(q, k, v, out_weight.T, post_gain[:, None], residual.T)
    return out.T


def general(positions, queries, keys, values, out_weight, post_gain, residual):
    rows = queries.shape[0]
    kv_heads = keys.shape[1]
    query_groups = QUERY_HEADS // KEY_VALUE_HEADS
    q_rot = rotate(queries, positions)
    stacked = jnp.stack([rotate(keys, positions), values], 0)
    reach = (VISIBLE_SPAN + rows - 2) // rows
    pieces = []
    carried = stacked
    for hop in range(reach):
        carried = passed_along(carried, "seq", 1)
        pieces.insert(0, carried)
    extended = jnp.concatenate(pieces + [stacked], axis=1)
    extra = extended.shape[1] - rows
    anchor = lax.axis_index("seq") * rows
    tile_rows = q_rot.reshape(rows, kv_heads, query_groups, -1)
    scores = jnp.einsum("qhgd,khd->hgqk", tile_rows, extended[0], preferred_element_type=jnp.float32) * SCALE
    query_index = anchor + jnp.arange(rows, dtype=jnp.int32)
    key_index = anchor - extra + jnp.arange(extra + rows, dtype=jnp.int32)
    gap = query_index[:, None] - key_index[None, :]
    allowed = (gap >= 0) & (gap < VISIBLE_SPAN) & (key_index[None, :] >= 0)
    scores = jnp.where(allowed, scores, MASKED)
    top = jnp.max(scores, axis=-1, keepdims=True)
    weights = jnp.exp(scores - top)
    probs = (weights / jnp.sum(weights, axis=-1, keepdims=True)).astype(jnp.bfloat16)
    context = jnp.einsum("hgqk,khd->qhgd", probs, extended[1], preferred_element_type=jnp.float32)
    context = context.astype(jnp.bfloat16).reshape(rows, -1)
    partial_value = jnp.dot(
        context,
        lax.all_gather(out_weight, "seq", axis=1, tiled=True),
        preferred_element_type=jnp.float32,
    )
    attended = lax.psum_scatter(
        partial_value.astype(jnp.bfloat16), "head", scatter_dimension=1, tiled=True
    ).astype(jnp.float32)
    squares = lax.psum(jnp.sum(attended * attended, axis=1), "head")
    scaled = attended * lax.rsqrt(squares / D + EPS)[:, None]
    result = residual.astype(jnp.float32) + post_gain[None, :] * scaled
    return result.astype(jnp.bfloat16)


def on_device(positions, queries, keys, values, out_weight, post_gain, residual):
    n_seq, n_head = lax.axis_size("seq"), lax.axis_size("head")
    rows, kv_heads, _ = keys.shape
    body = fused if fits(rows, out_weight.shape[0], kv_heads, queries.shape[1] // kv_heads, out_weight.shape[1], n_seq, n_head) else general
    return body(positions, queries, keys, values, out_weight, post_gain, residual)


def solution(mesh):
    return jax.shard_map(
        on_device,
        mesh=mesh,
        in_specs=(
            P("seq"),
            P("seq", "head", None),
            P("seq", "head", None),
            P("seq", "head", None),
            P("head", "seq"),
            P("head"),
            P("seq", "head"),
        ),
        out_specs=P("seq", "head"),
        check_vma=False,
    )
```

```python
import functools

import jax
import jax.numpy as jnp
from jax import lax
from jax.experimental import pallas as pl
from jax.experimental.pallas import tpu as pltpu
from jax.sharding import PartitionSpec as P

D = 5376
QUERY_HEADS = 32
KEY_VALUE_HEADS = 16
VISIBLE_SPAN = 1024


EPS = 1e-06
SCALE = 168.0 ** (-0.5)
LOG2E = 1.4426950408889634
MASKED = -1e30
TILE = 256
LANES = 128
MESH = pl.DeviceIdType.MESH
LAUNCH = (
    "Z0", "Z2", "Z3", "Z4", "Z5", "Z6", "H0", "H1", "H2", "H3", "Z1",
)
PLAN = (
    "T6", "T0", "T1", "T2", "T3", "T4", "T5", "C0", "A0", "A1", "C1", "A2",
    "A3", "C2", "C3", "R10", "R11", "R12", "R13", "X0", "Y0", "D0", "S0", "P002",
    "R20", "R21", "P022", "R22", "R23", "R31", "X1", "Y1", "D1", "S1", "P102", "R30",
    "P122", "R32", "R33", "X2", "Y2", "D2", "S2", "P202", "P222", "X3", "Y3", "D3",
    "S3", "P302", "P32", "P33",
)
DIRECT = (0, 1, 2, 3, )


def passed_along(value, axis, steps):
    count = lax.axis_size(axis)
    initial, last = (max(0, -steps), min(count, count - steps))
    return lax.ppermute(value, axis, [(source, source + steps) for source in range(initial, last)])


def rotate(x, positions):
    half = x.shape[-1] // 2
    inverse = 10000.0 ** (-2.0 * jnp.arange(half, dtype=jnp.float32) / x.shape[-1])
    angle = positions.astype(jnp.float32)[:, None] * inverse[None, :]
    cosine = jnp.concatenate([jnp.cos(angle), jnp.cos(angle)], -1)[:, None, :]
    sine = jnp.concatenate([jnp.sin(angle), jnp.sin(angle)], -1)[:, None, :]
    source = x.astype(jnp.float32)
    turned = jnp.concatenate([-source[..., half:], source[..., :half]], -1)
    return (source * cosine + turned * sine).astype(jnp.bfloat16)


def layer_kernel(
    n_seq, n_head, kv_heads, groups, reach,
    q_hbm, k_hbm, v_hbm, cos_hbm, sin_hbm, w_hbm, gain_hbm, res_hbm, out_ref,
    q_raw, k_raw, v_raw, cos_ref, sin_ref, w_ref, gain_ref, res_ref, load_sem,
    q_ref, gain_col, k_ext, v_ext, stage, w_all, ctx, acc, squares,
    halo_send, halo_recv, pass_send, a_send, a_recv, own_sem, c_send, c_recv,
    unit_send, forward_send, relay_send, unit_recv,
    up_send, down_send, ctx_recv, sq_send, sq_recv,
):
    me = lax.axis_index("seq")
    z = lax.axis_index("head")
    rows = k_raw.shape[0]
    size = k_raw.shape[2]
    feats = w_ref.shape[0]
    sub = n_seq // n_head
    span = reach * rows
    core = lax.rem(me, 2)
    chip = me // 2
    even = core == 0
    sibling = me + 1 - 2 * core
    across = me + 2 - 4 * lax.rem(chip, 2)
    along = me + 4 - 8 * (chip // 2)
    corner = across + along - me
    pair = groups * size

    def remote(src, dst, send, recv, device):
        return pltpu.make_async_remote_copy(
            src_ref=src, dst_ref=dst, send_sem=send, recv_sem=recv,
            device_id=device, device_id_type=MESH,
        )

    def order(s):
        low = z < n_head // 2
        near = jnp.where(low, z, n_head - 1 - z)
        at = near if s == 0 else (1 - near if s == 1 else s)
        return jnp.where(low, at, n_head - 1 - at)

    def halo(dist, g, kv, target):
        at, own = pl.ds(span - dist * rows, rows), pl.ds(span, rows)
        if kv == 0:
            src, dst = k_ext.at[g, own, :], k_ext.at[g, at, :]
        else:
            src, dst = v_ext.at[g, :, own], v_ext.at[g, :, at]
        return remote(src, dst, halo_send.at[dist - 1, g, kv], halo_recv.at[dist - 1, g, kv], (target, z))

    def passed_on(g, kv):
        near, far = pl.ds(span - rows, rows), pl.ds(span - 2 * rows, rows)
        if kv == 0:
            src, dst = k_ext.at[g, near, :], k_ext.at[g, far, :]
        else:
            src, dst = v_ext.at[g, :, near], v_ext.at[g, :, far]
        return remote(src, dst, pass_send.at[g, kv], halo_recv.at[1, g, kv], (me + 1, z))

    def start_halo(g):
        @pl.when(me + 1 < n_seq)
        def _():
            halo(1, g, 0, me + 1).start()
            halo(1, g, 1, me + 1).start()

        @pl.when(jnp.logical_and(even, me + 2 < n_seq))
        def _():
            halo(2, g, 0, me + 2).start()
            halo(2, g, 1, me + 2).start()

    def columns(target):
        return w_ref.at[:, pl.ds(pl.multiple_of(target * LANES, LANES), LANES)]

    def piece(source, target, direct):
        dst = w_all.at[target, z, lax.rem(source, sub)] if direct else stage.at[source]
        return remote(columns(target), dst, a_send.at[target], a_recv.at[source], (target, z))

    def scatter(target):
        @pl.when(me // sub == z)
        def _():
            piece(me, target, True).start()

        @pl.when(me // sub != z)
        def _():
            piece(me, target, False).start()

    def own_copy():
        return pltpu.make_async_copy(columns(me), w_all.at[me, z, lax.rem(me, sub)], own_sem)

    def own_climb():
        return remote(
            columns(me), w_all.at[me, z, lax.rem(me, sub)],
            c_send.at[me], c_recv.at[z, lax.rem(me, sub)], (me, me // sub),
        )

    def climb(source):
        return remote(
            stage.at[source], w_all.at[me, z, lax.rem(source, sub)],
            c_send.at[source], c_recv.at[z, lax.rem(source, sub)], (me, source // sub),
        )

    def take_piece(source):
        piece(source, me, False).wait_recv()

        @pl.when(source // sub != z)
        def _():
            climb(source).start()

    others = (across, along, across + 1 - 2 * core, along + 1 - 2 * core, corner, corner + 1 - 2 * core, sibling)

    def unit(owner, r, send, target):
        return remote(w_all.at[owner, r], w_all.at[owner, r], send, unit_recv.at[owner, r], (target, z))

    def send_unit(s):
        r = order(s)
        if s == 0:
            @pl.when(me // sub == z)
            def _():
                own_copy().wait()

        else:
            for j in range(sub):
                remote(stage.at[0], w_all.at[me, r, j], c_send.at[0], c_recv.at[r, j], (me, r)).wait_recv()
        unit(me, r, unit_send.at[0, s], across).start()
        unit(me, r, unit_send.at[1, s], along).start()
        if s in DIRECT:
            unit(me, r, forward_send.at[s], corner).start()
        unit(me, r, relay_send.at[0, s], sibling).start()

    def take_across(s):
        r = order(s)
        unit(across, r, unit_send.at[0, s], me).wait_recv()

        @pl.when(jnp.logical_and(even, s not in DIRECT))
        def _():
            unit(across, r, forward_send.at[s], along).start()

        unit(across, r, relay_send.at[1, s], sibling).start()

    def take_along(s):
        r = order(s)
        unit(along, r, unit_send.at[0, s], me).wait_recv()

        @pl.when(jnp.logical_and(jnp.logical_not(even), s not in DIRECT))
        def _():
            unit(along, r, forward_send.at[s], across).start()

        unit(along, r, relay_send.at[2, s], sibling).start()

    def take_corner(s):
        r = order(s)
        unit(corner, r, unit_send.at[0, s], me).wait_recv()
        unit(corner, r, relay_send.at[3, s], sibling).start()

    def take_relayed(s):
        r = order(s)
        for owner in (me, across, along, corner):
            unit(owner + 1 - 2 * core, r, unit_send.at[0, s], me).wait_recv()

    def chunk(r, g):
        return ctx.at[r, pl.ds(g * pair, pair), :]

    def ctx_up(r, g):
        return remote(chunk(r, g), chunk(r, g), up_send.at[r, g], ctx_recv.at[r, g], (me, z + 1))

    def ctx_down(r, g):
        return remote(chunk(r, g), chunk(r, g), down_send.at[r, g], ctx_recv.at[r, g], (me, z - 1))

    inner = jnp.logical_and(z >= 1, z + 1 < n_head)

    def arrive(s, g):
        r = order(s)

        @pl.when(inner)
        def _():
            ctx_up(r, g).wait_recv()

        @pl.when(jnp.logical_and(inner, r < z))
        def _():
            ctx_up(r, g).start()

        @pl.when(jnp.logical_and(inner, r > z))
        def _():
            ctx_down(r, g).start()

    blocks = span // TILE + 1

    def attend(g):
        for dist in range(1, reach + 1):
            @pl.when(me >= dist)
            def _():
                halo(dist, g, 0, me).wait_recv()
                halo(dist, g, 1, me).wait_recv()
                if dist == 1:
                    @pl.when(even)
                    def _():
                        passed_on(g, 0).start()
                        passed_on(g, 1).start()

        @pl.loop(0, rows // TILE)
        def _(t):
            first = pl.multiple_of(t * TILE, TILE)
            q = jnp.concatenate([q_ref[g * groups + i, pl.ds(first, TILE), :] for i in range(groups)], 0)
            row = lax.broadcasted_iota(jnp.int32, (TILE, groups * TILE), 0)
            col = lax.rem(lax.broadcasted_iota(jnp.int32, (TILE, groups * TILE), 1), TILE)
            scores = []
            top = None
            for b in range(blocks):
                s = lax.dot_general(
                    k_ext[g, pl.ds(first + b * TILE, TILE), :], q,
                    (((1,), (1,)), ((), ())), preferred_element_type=jnp.float32,
                )
                valid = me * rows + first + b * TILE - span >= 0
                if b == 0:
                    s = jnp.where(jnp.logical_and(row > col, valid), s, MASKED)
                elif b == blocks - 1:
                    s = jnp.where(row <= col, s, MASKED)
                else:
                    s = jnp.where(valid, s, MASKED)
                scores.append(s)
                high = jnp.max(s, axis=0, keepdims=True)
                top = high if top is None else jnp.maximum(top, high)
            shift = top * (SCALE * LOG2E)
            total = None
            mixed = None
            for b in range(blocks):
                w = jnp.exp2(scores[b] * (SCALE * LOG2E) - shift)
                part_sum = jnp.sum(w, axis=0, keepdims=True)
                total = part_sum if total is None else total + part_sum
                o = jnp.dot(
                    v_ext[g, :, pl.ds(pl.multiple_of(first + b * TILE, TILE), TILE)], w.astype(jnp.bfloat16),
                    preferred_element_type=jnp.float32,
                )
                mixed = o if mixed is None else mixed + o
            result = (mixed / total).astype(jnp.bfloat16)
            for i in range(groups):
                ctx[z, pl.ds((g * groups + i) * size, size), pl.ds(first, TILE)] = result[:, i * TILE : (i + 1) * TILE]

        @pl.when(z + 1 < n_head)
        def _():
            ctx_up(z, g).start()

        @pl.when(z >= 1)
        def _():
            ctx_down(z, g).start()

    tile = next(t for t in range(256, 0, -16) if feats % t == 0)

    def project(s, g, n=1):
        r = order(s)
        if s > 0:
            @pl.when(jnp.logical_not(inner))
            def _():
                for i in range(n):
                    ctx_up(r, g + i).wait_recv()

        block = ctx[r, pl.ds(g * pair, n * pair), :]
        for j in range(sub):
            @pl.loop(0, feats // tile)
            def _(t):
                at = pl.ds(pl.multiple_of(t * tile, tile), tile)
                w = jnp.concatenate([w_all[g * groups + i, r, j, at, :] for i in range(n * groups)], 1)
                got = jnp.dot(w, block, preferred_element_type=jnp.float32)
                if s == 0 and g == 0:
                    acc[j, at, :] = got
                else:
                    acc[j, at, :] += got

    loads = [pltpu.make_async_copy(src, dst, load_sem.at[i]) for i, (src, dst) in enumerate((
        (k_hbm, k_raw), (v_hbm, v_raw), (cos_hbm, cos_ref), (sin_hbm, sin_ref),
        (w_hbm, w_ref), (q_hbm, q_raw), (gain_hbm, gain_ref), (res_hbm, res_ref),
    ))]
    barrier = pltpu.get_barrier_semaphore()
    for d in range(1, n_seq):
        pl.semaphore_signal(barrier, inc=1, device_id=(lax.rem(me + d, n_seq), z), device_id_type=MESH)
    for d in range(1, n_head):
        pl.semaphore_signal(barrier, inc=1, device_id=(me, lax.rem(z + d, n_head)), device_id_type=MESH)
    for load in loads:
        load.start()

    def turned(x):
        x = jnp.swapaxes(x.astype(jnp.float32), 0, 1)
        return (x * cosine[None] + pltpu.roll(x, size // 2, 2) * sine[None]).astype(jnp.bfloat16)

    part = rows // 4
    for load in loads[:4]:
        load.wait()
    for t in range(0, rows, part):
        cosine, sine = cos_ref[t : t + part, :], sin_ref[t : t + part, :]
        k_ext[:, span + t : span + t + part, :] = turned(k_raw[t : t + part])
    for g in range(kv_heads):
        v_ext[g, :, span : span + rows] = v_raw[:, g, :].T
    loads[4].wait()
    pl.semaphore_wait(barrier, n_seq + n_head - 2)

    @pl.when(me // sub == z)
    def _():
        own_copy().start()

    @pl.when(me // sub != z)
    def _():
        own_climb().start()

    for word in LAUNCH:
        if word[0] == "H":
            start_halo(int(word[1]))
        else:
            scatter(others[int(word[1])])

    loads[5].wait()
    for t in range(0, rows, part):
        cosine, sine = cos_ref[t : t + part, :], sin_ref[t : t + part, :]
        q_ref[:, t : t + part, :] = turned(q_raw[t : t + part])
    for dist in range(1, reach + 1):
        @pl.when(me < dist)
        def _():
            at = pl.ds(span - dist * rows, rows)
            k_ext[:, at, :] = jnp.zeros((kv_heads, rows, size), jnp.bfloat16)
            v_ext[:, :, at] = jnp.zeros((kv_heads, size, rows), jnp.bfloat16)
    loads[6].wait()
    for first in range(0, gain_ref.shape[1], LANES):
        count = min(LANES, gain_ref.shape[1] - first)
        gain_col[first : first + count, :] = jnp.broadcast_to(gain_ref[:, first : first + count], (LANES, count)).T

    def take(n):
        take_piece(others[n])

    steps = {"T": take, "A": attend, "C": send_unit, "X": take_across, "Y": take_along, "D": take_corner,
             "S": take_relayed, "R": arrive, "P": project}
    for word in PLAN:
        steps[word[0]](*[int(c) for c in word[1:]])

    mine = jnp.zeros((8, rows), jnp.float32)
    for j in range(sub):
        value = acc[j]
        mine = mine + jnp.sum((value * value).reshape(feats // 8, 8, rows), axis=0)
    squares[0] = mine

    def sq(d, target):
        return remote(squares.at[0], squares.at[d], sq_send.at[d - 1], sq_recv.at[d - 1], (me, target))

    for d in range(1, n_head):
        sq(d, lax.rem(z + d, n_head)).start()
    for d in range(1, n_head):
        sq(d, z).wait_recv()
    loads[7].wait()
    whole = jnp.sum(jnp.sum(squares[...], axis=0), axis=0, keepdims=True)
    inverse = lax.rsqrt(whole / (n_head * sub * feats) + EPS)
    for j in range(sub):
        at = pl.ds(j * feats, feats)
        gain = jnp.concatenate([gain_col[at, :]] * (rows // LANES), 1)
        out_ref[at, :] = (
            res_ref[at, :].astype(jnp.float32) + gain * (acc[j] * inverse)
        ).astype(jnp.bfloat16)

    for d in range(1, n_head):
        sq(d, z).wait_send()
    for g in range(kv_heads):
        for dist in range(1, reach + 1):
            leaves = me + dist < n_seq
            if dist == 2:
                leaves = jnp.logical_and(even, leaves)

            @pl.when(leaves)
            def _():
                halo(dist, g, 0, me).wait_send()
                halo(dist, g, 1, me).wait_send()

        @pl.when(jnp.logical_and(even, me >= 1))
        def _():
            passed_on(g, 0).wait_send()
            passed_on(g, 1).wait_send()
    for target in others:
        piece(me, target, False).wait_send()
        source = target

        @pl.when(source // sub != z)
        def _():
            climb(source).wait_send()

    @pl.when(me // sub != z)
    def _():
        own_climb().wait_send()
    for s in range(n_head):
        for way in range(2):
            unit(me, s, unit_send.at[way, s], me).wait_send()
        unit(me, s, forward_send.at[s], me).wait_send()
        for way in range(4):
            unit(me, s, relay_send.at[way, s], me).wait_send()
    for g in range(kv_heads):
        for r in range(n_head):
            @pl.when(jnp.logical_and(r <= z, z + 1 < n_head))
            def _():
                ctx_up(r, g).wait_send()

            @pl.when(jnp.logical_and(r >= z, z >= 1))
            def _():
                ctx_down(r, g).wait_send()


def fits(rows, heads_rows, kv_heads, groups, feats, n_seq, n_head):
    return (
        n_seq == 8
        and n_head in (2, 4)
        and groups == 2
        and heads_rows == n_seq * LANES
        and rows % TILE == 0
        and VISIBLE_SPAN == 2 * rows
        and kv_heads * groups == n_seq
        and feats % 16 == 0
    )


def fused(positions, queries, keys, values, out_weight, post_gain, residual):
    n_seq, n_head = lax.axis_size("seq"), lax.axis_size("head")
    rows, kv_heads, size = keys.shape
    groups = queries.shape[1] // kv_heads
    feats = out_weight.shape[1]
    width = residual.shape[1]
    sub = n_seq // n_head
    reach = VISIBLE_SPAN // rows
    half = size // 2
    inverse = 10000.0 ** (-2.0 * jnp.arange(half, dtype=jnp.float32) / size)
    angle = positions.astype(jnp.float32)[:, None] * inverse[None, :]
    cosine = jnp.concatenate([jnp.cos(angle), jnp.cos(angle)], -1)
    sine = jnp.concatenate([-jnp.sin(angle), jnp.sin(angle)], -1)
    bf16, f32 = jnp.bfloat16, jnp.float32
    dma = pltpu.SemaphoreType.DMA
    spec = pl.BlockSpec(memory_space=pltpu.VMEM)
    out = pl.pallas_call(
        functools.partial(layer_kernel, n_seq, n_head, kv_heads, groups, reach),
        out_shape=jax.ShapeDtypeStruct((width, rows), bf16),
        in_specs=[pl.BlockSpec(memory_space=pl.ANY)] * 8,
        out_specs=spec,
        scratch_shapes=[
            pltpu.VMEM(queries.shape, bf16), pltpu.VMEM(keys.shape, bf16), pltpu.VMEM(keys.shape, bf16),
            pltpu.VMEM((rows, size), f32), pltpu.VMEM((rows, size), f32), pltpu.VMEM(out_weight.shape[::-1], bf16),
            pltpu.VMEM((1, width), f32), pltpu.VMEM((width, rows), bf16), dma((8,)),
            pltpu.VMEM((kv_heads * groups, rows, size), bf16),
            pltpu.VMEM((width, LANES), f32),
            pltpu.VMEM((kv_heads, (reach + 1) * rows, size), bf16),
            pltpu.VMEM((kv_heads, size, (reach + 1) * rows), bf16),
            pltpu.VMEM((n_seq, feats, LANES), bf16),
            pltpu.VMEM((n_seq, n_head, sub, feats, LANES), bf16),
            pltpu.VMEM((n_head, kv_heads * groups * size, rows), bf16),
            pltpu.VMEM((sub, feats, rows), f32),
            pltpu.VMEM((n_head, 8, rows), f32),
            dma((reach, kv_heads, 2)), dma((reach, kv_heads, 2)), dma((kv_heads, 2)),
            dma((n_seq,)), dma((n_seq,)), dma, dma((n_seq,)), dma((n_head, sub)),
            dma((2, n_head)), dma((n_head,)), dma((4, n_head)), dma((n_seq, n_head)),
            dma((n_head, kv_heads)), dma((n_head, kv_heads)), dma((n_head, kv_heads)),
            dma((n_head,)), dma((n_head,)),
        ],
        compiler_params=pltpu.CompilerParams(has_side_effects=True, collective_id=0, vmem_limit_bytes=44 * 1024 * 1024),
    )(queries, keys, values, cosine, sine, out_weight.T, post_gain[None, :], residual.T)
    return out.T


def general(positions, queries, keys, values, out_weight, post_gain, residual):
    rows = queries.shape[0]
    kv_heads = keys.shape[1]
    query_groups = QUERY_HEADS // KEY_VALUE_HEADS
    q_rot = rotate(queries, positions)
    stacked = jnp.stack([rotate(keys, positions), values], 0)
    reach = (VISIBLE_SPAN + rows - 2) // rows
    pieces = []
    carried = stacked
    for hop in range(reach):
        carried = passed_along(carried, "seq", 1)
        pieces.insert(0, carried)
    extended = jnp.concatenate(pieces + [stacked], axis=1)
    extra = extended.shape[1] - rows
    anchor = lax.axis_index("seq") * rows
    tile_rows = q_rot.reshape(rows, kv_heads, query_groups, -1)
    scores = jnp.einsum("qhgd,khd->hgqk", tile_rows, extended[0], preferred_element_type=jnp.float32) * SCALE
    query_index = anchor + jnp.arange(rows, dtype=jnp.int32)
    key_index = anchor - extra + jnp.arange(extra + rows, dtype=jnp.int32)
    gap = query_index[:, None] - key_index[None, :]
    allowed = (gap >= 0) & (gap < VISIBLE_SPAN) & (key_index[None, :] >= 0)
    scores = jnp.where(allowed, scores, MASKED)
    top = jnp.max(scores, axis=-1, keepdims=True)
    weights = jnp.exp(scores - top)
    probs = (weights / jnp.sum(weights, axis=-1, keepdims=True)).astype(jnp.bfloat16)
    context = jnp.einsum("hgqk,khd->qhgd", probs, extended[1], preferred_element_type=jnp.float32)
    context = context.astype(jnp.bfloat16).reshape(rows, -1)
    partial_value = jnp.dot(
        context,
        lax.all_gather(out_weight, "seq", axis=1, tiled=True),
        preferred_element_type=jnp.float32,
    )
    attended = lax.psum_scatter(
        partial_value.astype(jnp.bfloat16), "head", scatter_dimension=1, tiled=True
    ).astype(jnp.float32)
    squares = lax.psum(jnp.sum(attended * attended, axis=1), "head")
    scaled = attended * lax.rsqrt(squares / D + EPS)[:, None]
    result = residual.astype(jnp.float32) + post_gain[None, :] * scaled
    return result.astype(jnp.bfloat16)


def on_device(positions, queries, keys, values, out_weight, post_gain, residual):
    n_seq, n_head = lax.axis_size("seq"), lax.axis_size("head")
    rows, kv_heads, _ = keys.shape
    body = fused if fits(rows, out_weight.shape[0], kv_heads, queries.shape[1] // kv_heads, out_weight.shape[1], n_seq, n_head) else general
    return body(positions, queries, keys, values, out_weight, post_gain, residual)


def solution(mesh):
    return jax.shard_map(
        on_device,
        mesh=mesh,
        in_specs=(
            P("seq"),
            P("seq", "head", None),
            P("seq", "head", None),
            P("seq", "head", None),
            P("head", "seq"),
            P("head"),
            P("seq", "head"),
        ),
        out_specs=P("seq", "head"),
        check_vma=False,
    )
```

```python
import functools

import jax
import jax.numpy as jnp
from jax import lax
from jax.experimental import pallas as pl
from jax.experimental.pallas import tpu as pltpu
from jax.sharding import PartitionSpec as P

D = 5376
QUERY_HEADS = 32
KEY_VALUE_HEADS = 16
VISIBLE_SPAN = 1024


EPS = 1e-06
SCALE = 168.0 ** (-0.5)
LOG2E = 1.4426950408889634
MASKED = -1e30
TILE = 256
LANES = 128
MESH = pl.DeviceIdType.MESH
LAUNCH = (
    "Z4", "Z0", "Z1", "Z5", "Z2", "Z3", "Z6", "H0", "H1", "H2", "H3",
)
PLAN = (
    "T6", "T4", "T0", "T1", "T5", "T2", "T3", "C0", "A0", "A1", "A2", "A3",
    "C1", "C2", "C3", "R10", "R11", "R12", "R13", "X0", "Y0", "D0", "S0", "P002",
    "R20", "R21", "P022", "R22", "R23", "R31", "X1", "Y1", "D1", "S1", "P102", "R30",
    "P122", "R32", "R33", "X2", "Y2", "D2", "S2", "P202", "P222", "X3", "Y3", "D3",
    "S3", "P302", "P32", "P33",
)
DIRECT = (0, 1, 2, 3, )


def passed_along(value, axis, steps):
    count = lax.axis_size(axis)
    initial, last = (max(0, -steps), min(count, count - steps))
    return lax.ppermute(value, axis, [(source, source + steps) for source in range(initial, last)])


def rotate(x, positions):
    half = x.shape[-1] // 2
    inverse = 10000.0 ** (-2.0 * jnp.arange(half, dtype=jnp.float32) / x.shape[-1])
    angle = positions.astype(jnp.float32)[:, None] * inverse[None, :]
    cosine = jnp.concatenate([jnp.cos(angle), jnp.cos(angle)], -1)[:, None, :]
    sine = jnp.concatenate([jnp.sin(angle), jnp.sin(angle)], -1)[:, None, :]
    source = x.astype(jnp.float32)
    turned = jnp.concatenate([-source[..., half:], source[..., :half]], -1)
    return (source * cosine + turned * sine).astype(jnp.bfloat16)


def layer_kernel(
    n_seq, n_head, kv_heads, groups, reach,
    q_hbm, k_hbm, v_hbm, pos_hbm, rate_hbm, w_hbm, gain_hbm, res_hbm, out_ref,
    q_raw, k_raw, v_raw, pos_ref, rate_ref, w_ref, gain_ref, res_ref, load_sem,
    cos_ref, sin_ref,
    q_ref, gain_col, k_ext, v_ext, stage, w_all, ctx, acc, squares,
    halo_send, halo_recv, pass_send, a_send, a_recv, own_sem, c_send, c_recv,
    unit_send, forward_send, relay_send, unit_recv,
    up_send, down_send, ctx_recv, sq_send, sq_recv,
):
    me = lax.axis_index("seq")
    z = lax.axis_index("head")
    rows = k_raw.shape[0]
    size = k_raw.shape[2]
    feats = w_ref.shape[0]
    sub = n_seq // n_head
    span = reach * rows
    core = lax.rem(me, 2)
    chip = me // 2
    even = core == 0
    sibling = me + 1 - 2 * core
    across = me + 2 - 4 * lax.rem(chip, 2)
    along = me + 4 - 8 * (chip // 2)
    corner = across + along - me
    pair = groups * size

    def remote(src, dst, send, recv, device):
        return pltpu.make_async_remote_copy(
            src_ref=src, dst_ref=dst, send_sem=send, recv_sem=recv,
            device_id=device, device_id_type=MESH,
        )

    def order(s):
        low = z < n_head // 2
        near = jnp.where(low, z, n_head - 1 - z)
        at = near if s == 0 else (1 - near if s == 1 else s)
        return jnp.where(low, at, n_head - 1 - at)

    def halo(dist, g, kv, target):
        at, own = pl.ds(span - dist * rows, rows), pl.ds(span, rows)
        if kv == 0:
            src, dst = k_ext.at[g, own, :], k_ext.at[g, at, :]
        else:
            src, dst = v_ext.at[g, :, own], v_ext.at[g, :, at]
        return remote(src, dst, halo_send.at[dist - 1, g, kv], halo_recv.at[dist - 1, g, kv], (target, z))

    def passed_on(g, kv):
        near, far = pl.ds(span - rows, rows), pl.ds(span - 2 * rows, rows)
        if kv == 0:
            src, dst = k_ext.at[g, near, :], k_ext.at[g, far, :]
        else:
            src, dst = v_ext.at[g, :, near], v_ext.at[g, :, far]
        return remote(src, dst, pass_send.at[g, kv], halo_recv.at[1, g, kv], (me + 1, z))

    def start_halo(g):
        @pl.when(me + 1 < n_seq)
        def _():
            halo(1, g, 0, me + 1).start()
            halo(1, g, 1, me + 1).start()

        @pl.when(jnp.logical_and(even, me + 2 < n_seq))
        def _():
            halo(2, g, 0, me + 2).start()
            halo(2, g, 1, me + 2).start()

    def columns(target):
        return w_ref.at[:, pl.ds(pl.multiple_of(target * LANES, LANES), LANES)]

    def piece(source, target, direct):
        dst = w_all.at[target, z, lax.rem(source, sub)] if direct else stage.at[source]
        return remote(columns(target), dst, a_send.at[target], a_recv.at[source], (target, z))

    def scatter(target):
        @pl.when(me // sub == z)
        def _():
            piece(me, target, True).start()

        @pl.when(me // sub != z)
        def _():
            piece(me, target, False).start()

    def own_copy():
        return pltpu.make_async_copy(columns(me), w_all.at[me, z, lax.rem(me, sub)], own_sem)

    def own_climb():
        return remote(
            columns(me), w_all.at[me, z, lax.rem(me, sub)],
            c_send.at[me], c_recv.at[z, lax.rem(me, sub)], (me, me // sub),
        )

    def climb(source):
        return remote(
            stage.at[source], w_all.at[me, z, lax.rem(source, sub)],
            c_send.at[source], c_recv.at[z, lax.rem(source, sub)], (me, source // sub),
        )

    def take_piece(source):
        piece(source, me, False).wait_recv()

        @pl.when(source // sub != z)
        def _():
            climb(source).start()

    others = (across, along, across + 1 - 2 * core, along + 1 - 2 * core, corner, corner + 1 - 2 * core, sibling)

    def unit(owner, r, send, target):
        return remote(w_all.at[owner, r], w_all.at[owner, r], send, unit_recv.at[owner, r], (target, z))

    def send_unit(s):
        r = order(s)
        if s == 0:
            @pl.when(me // sub == z)
            def _():
                own_copy().wait()

        else:
            for j in range(sub):
                remote(stage.at[0], w_all.at[me, r, j], c_send.at[0], c_recv.at[r, j], (me, r)).wait_recv()
        unit(me, r, unit_send.at[0, s], across).start()
        unit(me, r, unit_send.at[1, s], along).start()
        if s in DIRECT:
            unit(me, r, forward_send.at[s], corner).start()
        unit(me, r, relay_send.at[0, s], sibling).start()

    def take_across(s):
        r = order(s)
        unit(across, r, unit_send.at[0, s], me).wait_recv()

        @pl.when(jnp.logical_and(even, s not in DIRECT))
        def _():
            unit(across, r, forward_send.at[s], along).start()

        unit(across, r, relay_send.at[1, s], sibling).start()

    def take_along(s):
        r = order(s)
        unit(along, r, unit_send.at[0, s], me).wait_recv()

        @pl.when(jnp.logical_and(jnp.logical_not(even), s not in DIRECT))
        def _():
            unit(along, r, forward_send.at[s], across).start()

        unit(along, r, relay_send.at[2, s], sibling).start()

    def take_corner(s):
        r = order(s)
        unit(corner, r, unit_send.at[0, s], me).wait_recv()
        unit(corner, r, relay_send.at[3, s], sibling).start()

    def take_relayed(s):
        r = order(s)
        for owner in (me, across, along, corner):
            unit(owner + 1 - 2 * core, r, unit_send.at[0, s], me).wait_recv()

    def chunk(r, g):
        return ctx.at[r, pl.ds(g * pair, pair), :]

    def ctx_up(r, g):
        return remote(chunk(r, g), chunk(r, g), up_send.at[r, g], ctx_recv.at[r, g], (me, z + 1))

    def ctx_down(r, g):
        return remote(chunk(r, g), chunk(r, g), down_send.at[r, g], ctx_recv.at[r, g], (me, z - 1))

    inner = jnp.logical_and(z >= 1, z + 1 < n_head)

    def arrive(s, g):
        r = order(s)

        @pl.when(inner)
        def _():
            ctx_up(r, g).wait_recv()

        @pl.when(jnp.logical_and(inner, r < z))
        def _():
            ctx_up(r, g).start()

        @pl.when(jnp.logical_and(inner, r > z))
        def _():
            ctx_down(r, g).start()

    blocks = span // TILE + 1

    def attend(g):
        for dist in range(1, reach + 1):
            @pl.when(me >= dist)
            def _():
                halo(dist, g, 0, me).wait_recv()
                halo(dist, g, 1, me).wait_recv()
                if dist == 1:
                    @pl.when(even)
                    def _():
                        passed_on(g, 0).start()
                        passed_on(g, 1).start()

        @pl.loop(0, rows // TILE)
        def _(t):
            first = pl.multiple_of(t * TILE, TILE)
            q = jnp.concatenate([q_ref[g * groups + i, pl.ds(first, TILE), :] for i in range(groups)], 0)
            row = lax.broadcasted_iota(jnp.int32, (TILE, groups * TILE), 0)
            col = lax.rem(lax.broadcasted_iota(jnp.int32, (TILE, groups * TILE), 1), TILE)
            scores = []
            top = None
            for b in range(blocks):
                s = lax.dot_general(
                    k_ext[g, pl.ds(first + b * TILE, TILE), :], q,
                    (((1,), (1,)), ((), ())), preferred_element_type=jnp.float32,
                )
                valid = me * rows + first + b * TILE - span >= 0
                if b == 0:
                    s = jnp.where(jnp.logical_and(row > col, valid), s, MASKED)
                elif b == blocks - 1:
                    s = jnp.where(row <= col, s, MASKED)
                else:
                    s = jnp.where(valid, s, MASKED)
                scores.append(s)
                high = jnp.max(s, axis=0, keepdims=True)
                top = high if top is None else jnp.maximum(top, high)
            shift = top * (SCALE * LOG2E)
            total = None
            mixed = None
            for b in range(blocks):
                w = jnp.exp2(scores[b] * (SCALE * LOG2E) - shift)
                part_sum = jnp.sum(w, axis=0, keepdims=True)
                total = part_sum if total is None else total + part_sum
                o = jnp.dot(
                    v_ext[g, :, pl.ds(pl.multiple_of(first + b * TILE, TILE), TILE)], w.astype(jnp.bfloat16),
                    preferred_element_type=jnp.float32,
                )
                mixed = o if mixed is None else mixed + o
            result = (mixed / total).astype(jnp.bfloat16)
            for i in range(groups):
                ctx[z, pl.ds((g * groups + i) * size, size), pl.ds(first, TILE)] = result[:, i * TILE : (i + 1) * TILE]

        @pl.when(z + 1 < n_head)
        def _():
            ctx_up(z, g).start()

        @pl.when(z >= 1)
        def _():
            ctx_down(z, g).start()

    tile = next(t for t in range(256, 0, -16) if feats % t == 0)

    def project(s, g, n=1):
        last = s == n_head - 1 and g + n == kv_heads
        r = order(s)
        if s > 0:
            @pl.when(jnp.logical_not(inner))
            def _():
                for i in range(n):
                    ctx_up(r, g + i).wait_recv()

        block = ctx[r, pl.ds(g * pair, n * pair), :]
        for j in range(sub):
            @pl.loop(0, feats // tile)
            def _(t):
                at = pl.ds(pl.multiple_of(t * tile, tile), tile)
                w = jnp.concatenate([w_all[g * groups + i, r, j, at, :] for i in range(n * groups)], 1)
                got = jnp.dot(w, block, preferred_element_type=jnp.float32)
                if s > 0 or g > 0:
                    got = got + acc[j, at, :]
                acc[j, at, :] = got
                if last:
                    squares[0] += jnp.sum((got * got).reshape(tile // 8, 8, rows), axis=0)

    loads = [pltpu.make_async_copy(src, dst, load_sem.at[i]) for i, (src, dst) in enumerate((
        (pos_hbm, pos_ref), (rate_hbm, rate_ref), (k_hbm, k_raw), (v_hbm, v_raw),
        (w_hbm, w_ref), (q_hbm, q_raw), (gain_hbm, gain_ref), (res_hbm, res_ref),
    ))]
    barrier = pltpu.get_barrier_semaphore()
    for d in range(1, n_seq):
        pl.semaphore_signal(barrier, inc=1, device_id=(lax.rem(me + d, n_seq), z), device_id_type=MESH)
    for d in range(1, n_head):
        pl.semaphore_signal(barrier, inc=1, device_id=(me, lax.rem(z + d, n_head)), device_id_type=MESH)
    for load in loads:
        load.start()

    def turned(x):
        x = jnp.swapaxes(x.astype(jnp.float32), 0, 1)
        return (x * cosine[None] + pltpu.roll(x, size // 2, 2) * sine[None]).astype(jnp.bfloat16)

    part = rows // 4
    for load in loads[:2]:
        load.wait()
    tokens = pos_ref[...].reshape(1, rows).astype(jnp.float32)
    early = lax.broadcasted_iota(jnp.int32, (size, size), 1) < size // 2
    for t in range(0, rows, size):
        angle = jnp.broadcast_to(tokens[:, t : t + size], (size, size)).T * rate_ref[...]
        cos_ref[t : t + size, :] = jnp.cos(angle)
        sine = jnp.sin(angle)
        sin_ref[t : t + size, :] = jnp.where(early, -sine, sine)
    for load in loads[2:4]:
        load.wait()
    for t in range(0, rows, part):
        cosine, sine = cos_ref[t : t + part, :], sin_ref[t : t + part, :]
        k_ext[:, span + t : span + t + part, :] = turned(k_raw[t : t + part])
    for g in range(kv_heads):
        v_ext[g, :, span : span + rows] = v_raw[:, g, :].T
    loads[4].wait()
    pl.semaphore_wait(barrier, n_seq + n_head - 2)

    @pl.when(me // sub == z)
    def _():
        own_copy().start()

    @pl.when(me // sub != z)
    def _():
        own_climb().start()

    for word in LAUNCH:
        if word[0] == "H":
            start_halo(int(word[1]))
        else:
            scatter(others[int(word[1])])

    squares[0] = jnp.zeros((8, rows), jnp.float32)
    loads[5].wait()
    for t in range(0, rows, part):
        cosine, sine = cos_ref[t : t + part, :], sin_ref[t : t + part, :]
        q_ref[:, t : t + part, :] = turned(q_raw[t : t + part])
    for dist in range(1, reach + 1):
        @pl.when(me < dist)
        def _():
            at = pl.ds(span - dist * rows, rows)
            k_ext[:, at, :] = jnp.zeros((kv_heads, rows, size), jnp.bfloat16)
            v_ext[:, :, at] = jnp.zeros((kv_heads, size, rows), jnp.bfloat16)
    loads[6].wait()
    gain_row = gain_ref[...].reshape(1, gain_ref.shape[0])
    for first in range(0, gain_ref.shape[0], LANES):
        count = min(LANES, gain_ref.shape[0] - first)
        gain_col[first : first + count, :] = jnp.broadcast_to(gain_row[:, first : first + count], (LANES, count)).T

    def take(n):
        take_piece(others[n])

    steps = {"T": take, "A": attend, "C": send_unit, "X": take_across, "Y": take_along, "D": take_corner,
             "S": take_relayed, "R": arrive, "P": project}
    for word in PLAN:
        steps[word[0]](*[int(c) for c in word[1:]])

    def sq(d, target):
        return remote(squares.at[0], squares.at[d], sq_send.at[d - 1], sq_recv.at[d - 1], (me, target))

    for d in range(1, n_head):
        sq(d, lax.rem(z + d, n_head)).start()
    for d in range(1, n_head):
        sq(d, z).wait_recv()
    loads[7].wait()
    whole = jnp.sum(jnp.sum(squares[...], axis=0), axis=0, keepdims=True)
    inverse = lax.rsqrt(whole / (n_head * sub * feats) + EPS)
    for j in range(sub):
        at = pl.ds(j * feats, feats)
        gain = jnp.concatenate([gain_col[at, :]] * (rows // LANES), 1)
        out_ref[at, :] = (
            res_ref[at, :].astype(jnp.float32) + gain * (acc[j] * inverse)
        ).astype(jnp.bfloat16)

    for d in range(1, n_head):
        sq(d, z).wait_send()
    for g in range(kv_heads):
        for dist in range(1, reach + 1):
            leaves = me + dist < n_seq
            if dist == 2:
                leaves = jnp.logical_and(even, leaves)

            @pl.when(leaves)
            def _():
                halo(dist, g, 0, me).wait_send()
                halo(dist, g, 1, me).wait_send()

        @pl.when(jnp.logical_and(even, me >= 1))
        def _():
            passed_on(g, 0).wait_send()
            passed_on(g, 1).wait_send()
    for target in others:
        piece(me, target, False).wait_send()
        source = target

        @pl.when(source // sub != z)
        def _():
            climb(source).wait_send()

    @pl.when(me // sub != z)
    def _():
        own_climb().wait_send()
    for s in range(n_head):
        for way in range(2):
            unit(me, s, unit_send.at[way, s], me).wait_send()
        unit(me, s, forward_send.at[s], me).wait_send()
        for way in range(4):
            unit(me, s, relay_send.at[way, s], me).wait_send()
    for g in range(kv_heads):
        for r in range(n_head):
            @pl.when(jnp.logical_and(r <= z, z + 1 < n_head))
            def _():
                ctx_up(r, g).wait_send()

            @pl.when(jnp.logical_and(r >= z, z >= 1))
            def _():
                ctx_down(r, g).wait_send()


def fits(rows, heads_rows, kv_heads, groups, feats, n_seq, n_head):
    return (
        n_seq == 8
        and n_head in (2, 4)
        and groups == 2
        and heads_rows == n_seq * LANES
        and rows % TILE == 0
        and VISIBLE_SPAN == 2 * rows
        and kv_heads * groups == n_seq
        and feats % 16 == 0
    )


def fused(positions, queries, keys, values, out_weight, post_gain, residual):
    n_seq, n_head = lax.axis_size("seq"), lax.axis_size("head")
    rows, kv_heads, size = keys.shape
    groups = queries.shape[1] // kv_heads
    feats = out_weight.shape[1]
    width = residual.shape[1]
    sub = n_seq // n_head
    reach = VISIBLE_SPAN // rows
    half = size // 2
    inverse = 10000.0 ** (-2.0 * jnp.arange(half, dtype=jnp.float32) / size)
    rate = jnp.concatenate([inverse, inverse])[None, :]
    bf16, f32 = jnp.bfloat16, jnp.float32
    dma = pltpu.SemaphoreType.DMA
    spec = pl.BlockSpec(memory_space=pltpu.VMEM)
    out = pl.pallas_call(
        functools.partial(layer_kernel, n_seq, n_head, kv_heads, groups, reach),
        out_shape=jax.ShapeDtypeStruct((width, rows), bf16),
        in_specs=[pl.BlockSpec(memory_space=pltpu.MemorySpace.HBM)] * 8,
        out_specs=spec,
        scratch_shapes=[
            pltpu.VMEM(queries.shape, bf16), pltpu.VMEM(keys.shape, bf16), pltpu.VMEM(keys.shape, bf16),
            pltpu.VMEM((rows,), jnp.int32), pltpu.VMEM((1, size), f32), pltpu.VMEM(out_weight.shape[::-1], bf16),
            pltpu.VMEM((width,), f32), pltpu.VMEM((width, rows), bf16), dma((8,)),
            pltpu.VMEM((rows, size), f32), pltpu.VMEM((rows, size), f32),
            pltpu.VMEM((kv_heads * groups, rows, size), bf16),
            pltpu.VMEM((width, LANES), f32),
            pltpu.VMEM((kv_heads, (reach + 1) * rows, size), bf16),
            pltpu.VMEM((kv_heads, size, (reach + 1) * rows), bf16),
            pltpu.VMEM((n_seq, feats, LANES), bf16),
            pltpu.VMEM((n_seq, n_head, sub, feats, LANES), bf16),
            pltpu.VMEM((n_head, kv_heads * groups * size, rows), bf16),
            pltpu.VMEM((sub, feats, rows), f32),
            pltpu.VMEM((n_head, 8, rows), f32),
            dma((reach, kv_heads, 2)), dma((reach, kv_heads, 2)), dma((kv_heads, 2)),
            dma((n_seq,)), dma((n_seq,)), dma, dma((n_seq,)), dma((n_head, sub)),
            dma((2, n_head)), dma((n_head,)), dma((4, n_head)), dma((n_seq, n_head)),
            dma((n_head, kv_heads)), dma((n_head, kv_heads)), dma((n_head, kv_heads)),
            dma((n_head,)), dma((n_head,)),
        ],
        compiler_params=pltpu.CompilerParams(has_side_effects=True, collective_id=0, vmem_limit_bytes=44 * 1024 * 1024),
    )(*[pltpu.with_memory_space_constraint(x, pltpu.MemorySpace.HBM) for x in (queries, keys, values, positions, rate, out_weight.T, post_gain, residual.T)])
    return out.T


def general(positions, queries, keys, values, out_weight, post_gain, residual):
    rows = queries.shape[0]
    kv_heads = keys.shape[1]
    query_groups = QUERY_HEADS // KEY_VALUE_HEADS
    q_rot = rotate(queries, positions)
    stacked = jnp.stack([rotate(keys, positions), values], 0)
    reach = (VISIBLE_SPAN + rows - 2) // rows
    pieces = []
    carried = stacked
    for hop in range(reach):
        carried = passed_along(carried, "seq", 1)
        pieces.insert(0, carried)
    extended = jnp.concatenate(pieces + [stacked], axis=1)
    extra = extended.shape[1] - rows
    anchor = lax.axis_index("seq") * rows
    tile_rows = q_rot.reshape(rows, kv_heads, query_groups, -1)
    scores = jnp.einsum("qhgd,khd->hgqk", tile_rows, extended[0], preferred_element_type=jnp.float32) * SCALE
    query_index = anchor + jnp.arange(rows, dtype=jnp.int32)
    key_index = anchor - extra + jnp.arange(extra + rows, dtype=jnp.int32)
    gap = query_index[:, None] - key_index[None, :]
    allowed = (gap >= 0) & (gap < VISIBLE_SPAN) & (key_index[None, :] >= 0)
    scores = jnp.where(allowed, scores, MASKED)
    top = jnp.max(scores, axis=-1, keepdims=True)
    weights = jnp.exp(scores - top)
    probs = (weights / jnp.sum(weights, axis=-1, keepdims=True)).astype(jnp.bfloat16)
    context = jnp.einsum("hgqk,khd->qhgd", probs, extended[1], preferred_element_type=jnp.float32)
    context = context.astype(jnp.bfloat16).reshape(rows, -1)
    partial_value = jnp.dot(
        context,
        lax.all_gather(out_weight, "seq", axis=1, tiled=True),
        preferred_element_type=jnp.float32,
    )
    attended = lax.psum_scatter(
        partial_value.astype(jnp.bfloat16), "head", scatter_dimension=1, tiled=True
    ).astype(jnp.float32)
    squares = lax.psum(jnp.sum(attended * attended, axis=1), "head")
    scaled = attended * lax.rsqrt(squares / D + EPS)[:, None]
    result = residual.astype(jnp.float32) + post_gain[None, :] * scaled
    return result.astype(jnp.bfloat16)


def on_device(positions, queries, keys, values, out_weight, post_gain, residual):
    n_seq, n_head = lax.axis_size("seq"), lax.axis_size("head")
    rows, kv_heads, _ = keys.shape
    body = fused if fits(rows, out_weight.shape[0], kv_heads, queries.shape[1] // kv_heads, out_weight.shape[1], n_seq, n_head) else general
    return body(positions, queries, keys, values, out_weight, post_gain, residual)


def solution(mesh):
    return jax.shard_map(
        on_device,
        mesh=mesh,
        in_specs=(
            P("seq"),
            P("seq", "head", None),
            P("seq", "head", None),
            P("seq", "head", None),
            P("head", "seq"),
            P("head"),
            P("seq", "head"),
        ),
        out_specs=P("seq", "head"),
        check_vma=False,
    )
```

```python
import functools

import jax
import jax.numpy as jnp
from jax import lax
from jax.experimental import pallas as pl
from jax.experimental.pallas import tpu as pltpu
from jax.sharding import PartitionSpec as P

D = 5376
QUERY_HEADS = 32
KEY_VALUE_HEADS = 16
VISIBLE_SPAN = 1024


EPS = 1e-06
SCALE = 168.0 ** (-0.5)
LOG2E = 1.4426950408889634
MASKED = -1e30
TILE = 256
LANES = 128
MESH = pl.DeviceIdType.MESH
LAUNCH = (
    "Z4", "Z0", "Z1", "Z5", "Z2", "Z3", "Z6", "H0", "H1", "H2", "H3",
)
PLAN = (
    "T6", "T4", "T0", "T1", "T5", "T2", "T3", "C0", "A0", "A1", "A2", "A3",
    "C1", "C2", "C3", "R10", "R11", "R12", "R13", "R20", "R21", "X0", "Y0", "D0",
    "S0", "P004", "R22", "R23", "R30", "R31", "X1", "Y1", "D1", "S1", "P104", "R32",
    "R33", "X2", "Y2", "D2", "S2", "P204", "X3", "Y3", "D3", "S3", "P303", "P33",
)
DIRECT = (0, 1, 2, 3, )


def passed_along(value, axis, steps):
    count = lax.axis_size(axis)
    initial, last = (max(0, -steps), min(count, count - steps))
    return lax.ppermute(value, axis, [(source, source + steps) for source in range(initial, last)])


def rotate(x, positions):
    half = x.shape[-1] // 2
    inverse = 10000.0 ** (-2.0 * jnp.arange(half, dtype=jnp.float32) / x.shape[-1])
    angle = positions.astype(jnp.float32)[:, None] * inverse[None, :]
    cosine = jnp.concatenate([jnp.cos(angle), jnp.cos(angle)], -1)[:, None, :]
    sine = jnp.concatenate([jnp.sin(angle), jnp.sin(angle)], -1)[:, None, :]
    source = x.astype(jnp.float32)
    turned = jnp.concatenate([-source[..., half:], source[..., :half]], -1)
    return (source * cosine + turned * sine).astype(jnp.bfloat16)


def layer_kernel(
    n_seq, n_head, kv_heads, groups, reach,
    q_hbm, k_hbm, v_hbm, pos_hbm, rate_hbm, w_hbm, gain_hbm, res_hbm, out_ref,
    q_raw, k_raw, v_raw, pos_ref, rate_ref, w_ref, gain_ref, res_ref, load_sem,
    cos_ref, sin_ref,
    q_ref, gain_col, k_ext, v_ext, stage, w_all, ctx, acc, squares,
    halo_send, halo_recv, pass_send, a_send, a_recv, own_sem, c_send, c_recv,
    unit_send, forward_send, relay_send, unit_recv,
    up_send, down_send, ctx_recv, sq_send, sq_recv,
):
    me = lax.axis_index("seq")
    z = lax.axis_index("head")
    rows = k_raw.shape[0]
    size = k_raw.shape[2]
    feats = w_ref.shape[0]
    sub = n_seq // n_head
    span = reach * rows
    core = lax.rem(me, 2)
    chip = me // 2
    even = core == 0
    sibling = me + 1 - 2 * core
    across = me + 2 - 4 * lax.rem(chip, 2)
    along = me + 4 - 8 * (chip // 2)
    corner = across + along - me
    pair = groups * size

    def remote(src, dst, send, recv, device):
        return pltpu.make_async_remote_copy(
            src_ref=src, dst_ref=dst, send_sem=send, recv_sem=recv,
            device_id=device, device_id_type=MESH,
        )

    def order(s):
        low = z < n_head // 2
        near = jnp.where(low, z, n_head - 1 - z)
        at = near if s == 0 else (1 - near if s == 1 else s)
        return jnp.where(low, at, n_head - 1 - at)

    def halo(dist, g, kv, target):
        at, own = pl.ds(span - dist * rows, rows), pl.ds(span, rows)
        if kv == 0:
            src, dst = k_ext.at[g, own, :], k_ext.at[g, at, :]
        else:
            src, dst = v_ext.at[g, :, own], v_ext.at[g, :, at]
        return remote(src, dst, halo_send.at[dist - 1, g, kv], halo_recv.at[dist - 1, g, kv], (target, z))

    def passed_on(g, kv):
        near, far = pl.ds(span - rows, rows), pl.ds(span - 2 * rows, rows)
        if kv == 0:
            src, dst = k_ext.at[g, near, :], k_ext.at[g, far, :]
        else:
            src, dst = v_ext.at[g, :, near], v_ext.at[g, :, far]
        return remote(src, dst, pass_send.at[g, kv], halo_recv.at[1, g, kv], (me + 1, z))

    def start_halo(g):
        @pl.when(me + 1 < n_seq)
        def _():
            halo(1, g, 0, me + 1).start()
            halo(1, g, 1, me + 1).start()

        @pl.when(jnp.logical_and(even, me + 2 < n_seq))
        def _():
            halo(2, g, 0, me + 2).start()
            halo(2, g, 1, me + 2).start()

    def columns(target):
        return w_ref.at[:, pl.ds(pl.multiple_of(target * LANES, LANES), LANES)]

    def piece(source, target, direct):
        dst = w_all.at[target, z, lax.rem(source, sub)] if direct else stage.at[source]
        return remote(columns(target), dst, a_send.at[target], a_recv.at[source], (target, z))

    def scatter(target):
        @pl.when(me // sub == z)
        def _():
            piece(me, target, True).start()

        @pl.when(me // sub != z)
        def _():
            piece(me, target, False).start()

    def own_copy():
        return pltpu.make_async_copy(columns(me), w_all.at[me, z, lax.rem(me, sub)], own_sem)

    def own_climb():
        return remote(
            columns(me), w_all.at[me, z, lax.rem(me, sub)],
            c_send.at[me], c_recv.at[z, lax.rem(me, sub)], (me, me // sub),
        )

    def climb(source):
        return remote(
            stage.at[source], w_all.at[me, z, lax.rem(source, sub)],
            c_send.at[source], c_recv.at[z, lax.rem(source, sub)], (me, source // sub),
        )

    def take_piece(source):
        piece(source, me, False).wait_recv()

        @pl.when(source // sub != z)
        def _():
            climb(source).start()

    others = (across, along, across + 1 - 2 * core, along + 1 - 2 * core, corner, corner + 1 - 2 * core, sibling)

    def unit(owner, r, send, target):
        return remote(w_all.at[owner, r], w_all.at[owner, r], send, unit_recv.at[owner, r], (target, z))

    def send_unit(s):
        r = order(s)
        if s == 0:
            @pl.when(me // sub == z)
            def _():
                own_copy().wait()

        else:
            for j in range(sub):
                remote(stage.at[0], w_all.at[me, r, j], c_send.at[0], c_recv.at[r, j], (me, r)).wait_recv()
        unit(me, r, unit_send.at[0, s], across).start()
        unit(me, r, unit_send.at[1, s], along).start()
        if s in DIRECT:
            unit(me, r, forward_send.at[s], corner).start()
        unit(me, r, relay_send.at[0, s], sibling).start()

    def take_across(s):
        r = order(s)
        unit(across, r, unit_send.at[0, s], me).wait_recv()

        @pl.when(jnp.logical_and(even, s not in DIRECT))
        def _():
            unit(across, r, forward_send.at[s], along).start()

        unit(across, r, relay_send.at[1, s], sibling).start()

    def take_along(s):
        r = order(s)
        unit(along, r, unit_send.at[0, s], me).wait_recv()

        @pl.when(jnp.logical_and(jnp.logical_not(even), s not in DIRECT))
        def _():
            unit(along, r, forward_send.at[s], across).start()

        unit(along, r, relay_send.at[2, s], sibling).start()

    def take_corner(s):
        r = order(s)
        unit(corner, r, unit_send.at[0, s], me).wait_recv()
        unit(corner, r, relay_send.at[3, s], sibling).start()

    def take_relayed(s):
        r = order(s)
        for owner in (me, across, along, corner):
            unit(owner + 1 - 2 * core, r, unit_send.at[0, s], me).wait_recv()

    def chunk(r, g):
        return ctx.at[r, pl.ds(g * pair, pair), :]

    def ctx_up(r, g):
        return remote(chunk(r, g), chunk(r, g), up_send.at[r, g], ctx_recv.at[r, g], (me, z + 1))

    def ctx_down(r, g):
        return remote(chunk(r, g), chunk(r, g), down_send.at[r, g], ctx_recv.at[r, g], (me, z - 1))

    inner = jnp.logical_and(z >= 1, z + 1 < n_head)

    def arrive(s, g):
        r = order(s)

        @pl.when(inner)
        def _():
            ctx_up(r, g).wait_recv()

        @pl.when(jnp.logical_and(inner, r < z))
        def _():
            ctx_up(r, g).start()

        @pl.when(jnp.logical_and(inner, r > z))
        def _():
            ctx_down(r, g).start()

    blocks = span // TILE + 1

    def attend(g):
        for dist in range(1, reach + 1):
            @pl.when(me >= dist)
            def _():
                halo(dist, g, 0, me).wait_recv()
                halo(dist, g, 1, me).wait_recv()
                if dist == 1:
                    @pl.when(even)
                    def _():
                        passed_on(g, 0).start()
                        passed_on(g, 1).start()

        @pl.loop(0, rows // TILE)
        def _(t):
            first = pl.multiple_of(t * TILE, TILE)
            q = jnp.concatenate([q_ref[g * groups + i, pl.ds(first, TILE), :] for i in range(groups)], 0)
            row = lax.broadcasted_iota(jnp.int32, (TILE, groups * TILE), 0)
            col = lax.rem(lax.broadcasted_iota(jnp.int32, (TILE, groups * TILE), 1), TILE)
            scores = []
            top = None
            for b in range(blocks):
                s = lax.dot_general(
                    k_ext[g, pl.ds(first + b * TILE, TILE), :], q,
                    (((1,), (1,)), ((), ())), preferred_element_type=jnp.float32,
                )
                valid = me * rows + first + b * TILE - span >= 0
                if b == 0:
                    s = jnp.where(jnp.logical_and(row > col, valid), s, MASKED)
                elif b == blocks - 1:
                    s = jnp.where(row <= col, s, MASKED)
                else:
                    s = jnp.where(valid, s, MASKED)
                scores.append(s)
                high = jnp.max(s, axis=0, keepdims=True)
                top = high if top is None else jnp.maximum(top, high)
            shift = top * (SCALE * LOG2E)
            total = None
            mixed = None
            for b in range(blocks):
                w = jnp.exp2(scores[b] * (SCALE * LOG2E) - shift)
                part_sum = jnp.sum(w, axis=0, keepdims=True)
                total = part_sum if total is None else total + part_sum
                o = jnp.dot(
                    v_ext[g, :, pl.ds(pl.multiple_of(first + b * TILE, TILE), TILE)], w.astype(jnp.bfloat16),
                    preferred_element_type=jnp.float32,
                )
                mixed = o if mixed is None else mixed + o
            result = (mixed / total).astype(jnp.bfloat16)
            for i in range(groups):
                ctx[z, pl.ds((g * groups + i) * size, size), pl.ds(first, TILE)] = result[:, i * TILE : (i + 1) * TILE]

        @pl.when(z + 1 < n_head)
        def _():
            ctx_up(z, g).start()

        @pl.when(z >= 1)
        def _():
            ctx_down(z, g).start()

    tile = next(t for t in range(256, 0, -16) if feats % t == 0)

    def project(s, g, n=1):
        last = s == n_head - 1 and g + n == kv_heads
        r = order(s)
        if s > 0:
            @pl.when(jnp.logical_not(inner))
            def _():
                for i in range(n):
                    ctx_up(r, g + i).wait_recv()

        block = ctx[r, pl.ds(g * pair, n * pair), :]
        for j in range(sub):
            @pl.loop(0, feats // tile)
            def _(t):
                at = pl.ds(pl.multiple_of(t * tile, tile), tile)
                w = jnp.concatenate([w_all[g * groups + i, r, j, at, :] for i in range(n * groups)], 1)
                got = jnp.dot(w, block, preferred_element_type=jnp.float32)
                if s > 0 or g > 0:
                    got = got + acc[j, at, :]
                acc[j, at, :] = got
                if last:
                    squares[0] += jnp.sum((got * got).reshape(tile // 8, 8, rows), axis=0)

    loads = [pltpu.make_async_copy(src, dst, load_sem.at[i]) for i, (src, dst) in enumerate((
        (pos_hbm, pos_ref), (rate_hbm, rate_ref), (k_hbm, k_raw), (v_hbm, v_raw),
        (w_hbm, w_ref), (q_hbm, q_raw), (gain_hbm, gain_ref), (res_hbm, res_ref),
    ))]
    barrier = pltpu.get_barrier_semaphore()
    for d in range(1, n_seq):
        pl.semaphore_signal(barrier, inc=1, device_id=(lax.rem(me + d, n_seq), z), device_id_type=MESH)
    for d in range(1, n_head):
        pl.semaphore_signal(barrier, inc=1, device_id=(me, lax.rem(z + d, n_head)), device_id_type=MESH)
    for load in loads:
        load.start()

    def turned(x):
        x = jnp.swapaxes(x.astype(jnp.float32), 0, 1)
        return (x * cosine[None] + pltpu.roll(x, size // 2, 2) * sine[None]).astype(jnp.bfloat16)

    part = rows // 4
    for load in loads[:2]:
        load.wait()
    tokens = pos_ref[...].reshape(1, rows).astype(jnp.float32)
    early = lax.broadcasted_iota(jnp.int32, (size, size), 1) < size // 2
    for t in range(0, rows, size):
        angle = jnp.broadcast_to(tokens[:, t : t + size], (size, size)).T * rate_ref[...]
        cos_ref[t : t + size, :] = jnp.cos(angle)
        sine = jnp.sin(angle)
        sin_ref[t : t + size, :] = jnp.where(early, -sine, sine)
    loads[4].wait()
    pl.semaphore_wait(barrier, n_seq + n_head - 2)

    @pl.when(me // sub == z)
    def _():
        own_copy().start()

    @pl.when(me // sub != z)
    def _():
        own_climb().start()

    for word in LAUNCH:
        if word[0] != "H":
            scatter(others[int(word[1])])
    for load in loads[2:4]:
        load.wait()
    for t in range(0, rows, part):
        cosine, sine = cos_ref[t : t + part, :], sin_ref[t : t + part, :]
        k_ext[:, span + t : span + t + part, :] = turned(k_raw[t : t + part])
    for g in range(kv_heads):
        v_ext[g, :, span : span + rows] = v_raw[:, g, :].T
    for g in range(kv_heads):
        start_halo(g)
    squares[0] = jnp.zeros((8, rows), jnp.float32)
    loads[5].wait()
    for t in range(0, rows, part):
        cosine, sine = cos_ref[t : t + part, :], sin_ref[t : t + part, :]
        q_ref[:, t : t + part, :] = turned(q_raw[t : t + part])
    for dist in range(1, reach + 1):
        @pl.when(me < dist)
        def _():
            at = pl.ds(span - dist * rows, rows)
            k_ext[:, at, :] = jnp.zeros((kv_heads, rows, size), jnp.bfloat16)
            v_ext[:, :, at] = jnp.zeros((kv_heads, size, rows), jnp.bfloat16)
    loads[6].wait()
    gain_row = gain_ref[...].reshape(1, gain_ref.shape[0])
    for first in range(0, gain_ref.shape[0], LANES):
        count = min(LANES, gain_ref.shape[0] - first)
        gain_col[first : first + count, :] = jnp.broadcast_to(gain_row[:, first : first + count], (LANES, count)).T

    def take(n):
        take_piece(others[n])

    steps = {"T": take, "A": attend, "C": send_unit, "X": take_across, "Y": take_along, "D": take_corner,
             "S": take_relayed, "R": arrive, "P": project}
    for word in PLAN:
        steps[word[0]](*[int(c) for c in word[1:]])

    def sq(d, target):
        return remote(squares.at[0], squares.at[d], sq_send.at[d - 1], sq_recv.at[d - 1], (me, target))

    for d in range(1, n_head):
        sq(d, lax.rem(z + d, n_head)).start()
    for d in range(1, n_head):
        sq(d, z).wait_recv()
    loads[7].wait()
    whole = jnp.sum(jnp.sum(squares[...], axis=0), axis=0, keepdims=True)
    inverse = lax.rsqrt(whole / (n_head * sub * feats) + EPS)
    for j in range(sub):
        at = pl.ds(j * feats, feats)
        gain = jnp.concatenate([gain_col[at, :]] * (rows // LANES), 1)
        out_ref[at, :] = (
            res_ref[at, :].astype(jnp.float32) + gain * (acc[j] * inverse)
        ).astype(jnp.bfloat16)

    for d in range(1, n_head):
        sq(d, z).wait_send()
    for g in range(kv_heads):
        for dist in range(1, reach + 1):
            leaves = me + dist < n_seq
            if dist == 2:
                leaves = jnp.logical_and(even, leaves)

            @pl.when(leaves)
            def _():
                halo(dist, g, 0, me).wait_send()
                halo(dist, g, 1, me).wait_send()

        @pl.when(jnp.logical_and(even, me >= 1))
        def _():
            passed_on(g, 0).wait_send()
            passed_on(g, 1).wait_send()
    for target in others:
        piece(me, target, False).wait_send()
        source = target

        @pl.when(source // sub != z)
        def _():
            climb(source).wait_send()

    @pl.when(me // sub != z)
    def _():
        own_climb().wait_send()
    for s in range(n_head):
        for way in range(2):
            unit(me, s, unit_send.at[way, s], me).wait_send()
        unit(me, s, forward_send.at[s], me).wait_send()
        for way in range(4):
            unit(me, s, relay_send.at[way, s], me).wait_send()
    for g in range(kv_heads):
        for r in range(n_head):
            @pl.when(jnp.logical_and(r <= z, z + 1 < n_head))
            def _():
                ctx_up(r, g).wait_send()

            @pl.when(jnp.logical_and(r >= z, z >= 1))
            def _():
                ctx_down(r, g).wait_send()


def fits(rows, heads_rows, kv_heads, groups, feats, n_seq, n_head):
    return (
        n_seq == 8
        and n_head in (2, 4)
        and groups == 2
        and heads_rows == n_seq * LANES
        and rows % TILE == 0
        and VISIBLE_SPAN == 2 * rows
        and kv_heads * groups == n_seq
        and feats % 16 == 0
    )


def fused(positions, queries, keys, values, out_weight, post_gain, residual):
    n_seq, n_head = lax.axis_size("seq"), lax.axis_size("head")
    rows, kv_heads, size = keys.shape
    groups = queries.shape[1] // kv_heads
    feats = out_weight.shape[1]
    width = residual.shape[1]
    sub = n_seq // n_head
    reach = VISIBLE_SPAN // rows
    half = size // 2
    inverse = 10000.0 ** (-2.0 * jnp.arange(half, dtype=jnp.float32) / size)
    rate = jnp.concatenate([inverse, inverse])[None, :]
    bf16, f32 = jnp.bfloat16, jnp.float32
    dma = pltpu.SemaphoreType.DMA
    spec = pl.BlockSpec(memory_space=pltpu.VMEM)
    out = pl.pallas_call(
        functools.partial(layer_kernel, n_seq, n_head, kv_heads, groups, reach),
        out_shape=jax.ShapeDtypeStruct((width, rows), bf16),
        in_specs=[pl.BlockSpec(memory_space=pltpu.MemorySpace.HBM)] * 8,
        out_specs=spec,
        scratch_shapes=[
            pltpu.VMEM(queries.shape, bf16), pltpu.VMEM(keys.shape, bf16), pltpu.VMEM(keys.shape, bf16),
            pltpu.VMEM((rows,), jnp.int32), pltpu.VMEM((1, size), f32), pltpu.VMEM(out_weight.shape[::-1], bf16),
            pltpu.VMEM((width,), f32), pltpu.VMEM((width, rows), bf16), dma((8,)),
            pltpu.VMEM((rows, size), f32), pltpu.VMEM((rows, size), f32),
            pltpu.VMEM((kv_heads * groups, rows, size), bf16),
            pltpu.VMEM((width, LANES), f32),
            pltpu.VMEM((kv_heads, (reach + 1) * rows, size), bf16),
            pltpu.VMEM((kv_heads, size, (reach + 1) * rows), bf16),
            pltpu.VMEM((n_seq, feats, LANES), bf16),
            pltpu.VMEM((n_seq, n_head, sub, feats, LANES), bf16),
            pltpu.VMEM((n_head, kv_heads * groups * size, rows), bf16),
            pltpu.VMEM((sub, feats, rows), f32),
            pltpu.VMEM((n_head, 8, rows), f32),
            dma((reach, kv_heads, 2)), dma((reach, kv_heads, 2)), dma((kv_heads, 2)),
            dma((n_seq,)), dma((n_seq,)), dma, dma((n_seq,)), dma((n_head, sub)),
            dma((2, n_head)), dma((n_head,)), dma((4, n_head)), dma((n_seq, n_head)),
            dma((n_head, kv_heads)), dma((n_head, kv_heads)), dma((n_head, kv_heads)),
            dma((n_head,)), dma((n_head,)),
        ],
        compiler_params=pltpu.CompilerParams(has_side_effects=True, collective_id=0, vmem_limit_bytes=44 * 1024 * 1024),
    )(*[pltpu.with_memory_space_constraint(x, pltpu.MemorySpace.HBM) for x in (queries, keys, values, positions, rate, out_weight.T, post_gain, residual.T)])
    return out.T


def general(positions, queries, keys, values, out_weight, post_gain, residual):
    rows = queries.shape[0]
    kv_heads = keys.shape[1]
    query_groups = QUERY_HEADS // KEY_VALUE_HEADS
    q_rot = rotate(queries, positions)
    stacked = jnp.stack([rotate(keys, positions), values], 0)
    reach = (VISIBLE_SPAN + rows - 2) // rows
    pieces = []
    carried = stacked
    for hop in range(reach):
        carried = passed_along(carried, "seq", 1)
        pieces.insert(0, carried)
    extended = jnp.concatenate(pieces + [stacked], axis=1)
    extra = extended.shape[1] - rows
    anchor = lax.axis_index("seq") * rows
    tile_rows = q_rot.reshape(rows, kv_heads, query_groups, -1)
    scores = jnp.einsum("qhgd,khd->hgqk", tile_rows, extended[0], preferred_element_type=jnp.float32) * SCALE
    query_index = anchor + jnp.arange(rows, dtype=jnp.int32)
    key_index = anchor - extra + jnp.arange(extra + rows, dtype=jnp.int32)
    gap = query_index[:, None] - key_index[None, :]
    allowed = (gap >= 0) & (gap < VISIBLE_SPAN) & (key_index[None, :] >= 0)
    scores = jnp.where(allowed, scores, MASKED)
    top = jnp.max(scores, axis=-1, keepdims=True)
    weights = jnp.exp(scores - top)
    probs = (weights / jnp.sum(weights, axis=-1, keepdims=True)).astype(jnp.bfloat16)
    context = jnp.einsum("hgqk,khd->qhgd", probs, extended[1], preferred_element_type=jnp.float32)
    context = context.astype(jnp.bfloat16).reshape(rows, -1)
    partial_value = jnp.dot(
        context,
        lax.all_gather(out_weight, "seq", axis=1, tiled=True),
        preferred_element_type=jnp.float32,
    )
    attended = lax.psum_scatter(
        partial_value.astype(jnp.bfloat16), "head", scatter_dimension=1, tiled=True
    ).astype(jnp.float32)
    squares = lax.psum(jnp.sum(attended * attended, axis=1), "head")
    scaled = attended * lax.rsqrt(squares / D + EPS)[:, None]
    result = residual.astype(jnp.float32) + post_gain[None, :] * scaled
    return result.astype(jnp.bfloat16)


def on_device(positions, queries, keys, values, out_weight, post_gain, residual):
    n_seq, n_head = lax.axis_size("seq"), lax.axis_size("head")
    rows, kv_heads, _ = keys.shape
    body = fused if fits(rows, out_weight.shape[0], kv_heads, queries.shape[1] // kv_heads, out_weight.shape[1], n_seq, n_head) else general
    return body(positions, queries, keys, values, out_weight, post_gain, residual)


def solution(mesh):
    return jax.shard_map(
        on_device,
        mesh=mesh,
        in_specs=(
            P("seq"),
            P("seq", "head", None),
            P("seq", "head", None),
            P("seq", "head", None),
            P("head", "seq"),
            P("head"),
            P("seq", "head"),
        ),
        out_specs=P("seq", "head"),
        check_vma=False,
    )
```

```python
import functools

import jax
import jax.numpy as jnp
from jax import lax
from jax.experimental import pallas as pl
from jax.experimental.pallas import tpu as pltpu
from jax.sharding import PartitionSpec as P

D = 5376
QUERY_HEADS = 32
KEY_VALUE_HEADS = 16
VISIBLE_SPAN = 1024


EPS = 1e-06
SCALE = 168.0 ** (-0.5)
LOG2E = 1.4426950408889634
MASKED = -1e30
TILE = 256
LANES = 128
MESH = pl.DeviceIdType.MESH
LAUNCH = (
    "Z4", "Z0", "Z1", "Z2", "Z3", "Z5", "Z6", "H0", "H1", "H2", "H3",
)
PLAN = (
    "T6", "T4", "T0", "T1", "T2", "T3", "T5", "C0", "A0", "A1", "A2", "A3",
    "C1", "C2", "C3", "R10", "R11", "R12", "R13", "R20", "R21", "X0", "Y0", "D0",
    "S0", "R22", "R23", "P004", "R30", "R31", "R32", "X1", "Y1", "D1", "S1", "P104",
    "R33", "X2", "Y2", "D2", "S2", "P204", "X3", "Y3", "D3", "S3", "P303", "P33",
)
DIRECT = (0, 1, 2, 3, )


def passed_along(value, axis, steps):
    count = lax.axis_size(axis)
    initial, last = (max(0, -steps), min(count, count - steps))
    return lax.ppermute(value, axis, [(source, source + steps) for source in range(initial, last)])


def rotate(x, positions):
    half = x.shape[-1] // 2
    inverse = 10000.0 ** (-2.0 * jnp.arange(half, dtype=jnp.float32) / x.shape[-1])
    angle = positions.astype(jnp.float32)[:, None] * inverse[None, :]
    cosine = jnp.concatenate([jnp.cos(angle), jnp.cos(angle)], -1)[:, None, :]
    sine = jnp.concatenate([jnp.sin(angle), jnp.sin(angle)], -1)[:, None, :]
    source = x.astype(jnp.float32)
    turned = jnp.concatenate([-source[..., half:], source[..., :half]], -1)
    return (source * cosine + turned * sine).astype(jnp.bfloat16)


def layer_kernel(
    n_seq, n_head, kv_heads, groups, reach,
    q_hbm, k_hbm, v_hbm, pos_hbm, rate_hbm, w_hbm, gain_hbm, res_hbm, out_ref,
    q_raw, k_raw, v_raw, pos_ref, rate_ref, w_ref, gain_ref, res_ref, load_sem,
    cos_ref, sin_ref,
    q_ref, gain_col, k_ext, v_ext, stage, w_all, ctx, acc, squares,
    halo_send, halo_recv, pass_send, a_send, a_recv, own_sem, c_send, c_recv,
    unit_send, forward_send, relay_send, unit_recv,
    up_send, down_send, ctx_recv, sq_send, sq_recv,
):
    me = lax.axis_index("seq")
    z = lax.axis_index("head")
    rows = k_raw.shape[0]
    size = k_raw.shape[2]
    feats = w_ref.shape[0]
    sub = n_seq // n_head
    span = reach * rows
    core = lax.rem(me, 2)
    chip = me // 2
    even = core == 0
    sibling = me + 1 - 2 * core
    across = me + 2 - 4 * lax.rem(chip, 2)
    along = me + 4 - 8 * (chip // 2)
    corner = across + along - me
    pair = groups * size

    def remote(src, dst, send, recv, device):
        return pltpu.make_async_remote_copy(
            src_ref=src, dst_ref=dst, send_sem=send, recv_sem=recv,
            device_id=device, device_id_type=MESH,
        )

    def order(s):
        low = z < n_head // 2
        near = jnp.where(low, z, n_head - 1 - z)
        at = near if s == 0 else (1 - near if s == 1 else s)
        return jnp.where(low, at, n_head - 1 - at)

    def halo(dist, g, kv, target):
        at, own = pl.ds(span - dist * rows, rows), pl.ds(span, rows)
        if kv == 0:
            src, dst = k_ext.at[g, own, :], k_ext.at[g, at, :]
        else:
            src, dst = v_ext.at[g, :, own], v_ext.at[g, :, at]
        return remote(src, dst, halo_send.at[dist - 1, g, kv], halo_recv.at[dist - 1, g, kv], (target, z))

    def passed_on(g, kv):
        near, far = pl.ds(span - rows, rows), pl.ds(span - 2 * rows, rows)
        if kv == 0:
            src, dst = k_ext.at[g, near, :], k_ext.at[g, far, :]
        else:
            src, dst = v_ext.at[g, :, near], v_ext.at[g, :, far]
        return remote(src, dst, pass_send.at[g, kv], halo_recv.at[1, g, kv], (me + 1, z))

    def start_halo(g):
        @pl.when(me + 1 < n_seq)
        def _():
            halo(1, g, 0, me + 1).start()
            halo(1, g, 1, me + 1).start()

        @pl.when(jnp.logical_and(even, me + 2 < n_seq))
        def _():
            halo(2, g, 0, me + 2).start()
            halo(2, g, 1, me + 2).start()

    def columns(target):
        return w_ref.at[:, pl.ds(pl.multiple_of(target * LANES, LANES), LANES)]

    def piece(source, target, direct):
        dst = w_all.at[target, z, lax.rem(source, sub)] if direct else stage.at[source]
        return remote(columns(target), dst, a_send.at[target], a_recv.at[source], (target, z))

    def scatter(target):
        @pl.when(me // sub == z)
        def _():
            piece(me, target, True).start()

        @pl.when(me // sub != z)
        def _():
            piece(me, target, False).start()

    def own_copy():
        return pltpu.make_async_copy(columns(me), w_all.at[me, z, lax.rem(me, sub)], own_sem)

    def own_climb():
        return remote(
            columns(me), w_all.at[me, z, lax.rem(me, sub)],
            c_send.at[me], c_recv.at[z, lax.rem(me, sub)], (me, me // sub),
        )

    def climb(source):
        return remote(
            stage.at[source], w_all.at[me, z, lax.rem(source, sub)],
            c_send.at[source], c_recv.at[z, lax.rem(source, sub)], (me, source // sub),
        )

    def take_piece(source):
        piece(source, me, False).wait_recv()

        @pl.when(source // sub != z)
        def _():
            climb(source).start()

    others = (across, along, across + 1 - 2 * core, along + 1 - 2 * core, corner, corner + 1 - 2 * core, sibling)

    def unit(owner, r, send, target):
        return remote(w_all.at[owner, r], w_all.at[owner, r], send, unit_recv.at[owner, r], (target, z))

    def send_unit(s):
        r = order(s)
        if s == 0:
            @pl.when(me // sub == z)
            def _():
                own_copy().wait()

        else:
            for j in range(sub):
                remote(stage.at[0], w_all.at[me, r, j], c_send.at[0], c_recv.at[r, j], (me, r)).wait_recv()
        unit(me, r, unit_send.at[0, s], across).start()
        unit(me, r, unit_send.at[1, s], along).start()
        if s in DIRECT:
            unit(me, r, forward_send.at[s], corner).start()
        unit(me, r, relay_send.at[0, s], sibling).start()

    def take_across(s):
        r = order(s)
        unit(across, r, unit_send.at[0, s], me).wait_recv()

        @pl.when(jnp.logical_and(even, s not in DIRECT))
        def _():
            unit(across, r, forward_send.at[s], along).start()

        unit(across, r, relay_send.at[1, s], sibling).start()

    def take_along(s):
        r = order(s)
        unit(along, r, unit_send.at[0, s], me).wait_recv()

        @pl.when(jnp.logical_and(jnp.logical_not(even), s not in DIRECT))
        def _():
            unit(along, r, forward_send.at[s], across).start()

        unit(along, r, relay_send.at[2, s], sibling).start()

    def take_corner(s):
        r = order(s)
        unit(corner, r, unit_send.at[0, s], me).wait_recv()
        unit(corner, r, relay_send.at[3, s], sibling).start()

    def take_relayed(s):
        r = order(s)
        for owner in (me, across, along, corner):
            unit(owner + 1 - 2 * core, r, unit_send.at[0, s], me).wait_recv()

    def chunk(r, g):
        return ctx.at[r, pl.ds(g * pair, pair), :]

    def ctx_up(r, g):
        return remote(chunk(r, g), chunk(r, g), up_send.at[r, g], ctx_recv.at[r, g], (me, z + 1))

    def ctx_down(r, g):
        return remote(chunk(r, g), chunk(r, g), down_send.at[r, g], ctx_recv.at[r, g], (me, z - 1))

    inner = jnp.logical_and(z >= 1, z + 1 < n_head)

    def arrive(s, g):
        r = order(s)

        @pl.when(inner)
        def _():
            ctx_up(r, g).wait_recv()

        @pl.when(jnp.logical_and(inner, r < z))
        def _():
            ctx_up(r, g).start()

        @pl.when(jnp.logical_and(inner, r > z))
        def _():
            ctx_down(r, g).start()

    blocks = span // TILE + 1

    def attend(g):
        for dist in range(1, reach + 1):
            @pl.when(me >= dist)
            def _():
                halo(dist, g, 0, me).wait_recv()
                halo(dist, g, 1, me).wait_recv()
                if dist == 1:
                    @pl.when(even)
                    def _():
                        passed_on(g, 0).start()
                        passed_on(g, 1).start()

        @pl.loop(0, rows // TILE)
        def _(t):
            first = pl.multiple_of(t * TILE, TILE)
            q = jnp.concatenate([q_ref[g * groups + i, pl.ds(first, TILE), :] for i in range(groups)], 0)
            row = lax.broadcasted_iota(jnp.int32, (TILE, groups * TILE), 0)
            col = lax.rem(lax.broadcasted_iota(jnp.int32, (TILE, groups * TILE), 1), TILE)
            scores = []
            top = None
            for b in range(blocks):
                s = lax.dot_general(
                    k_ext[g, pl.ds(first + b * TILE, TILE), :], q,
                    (((1,), (1,)), ((), ())), preferred_element_type=jnp.float32,
                )
                valid = me * rows + first + b * TILE - span >= 0
                if b == 0:
                    s = jnp.where(jnp.logical_and(row > col, valid), s, MASKED)
                elif b == blocks - 1:
                    s = jnp.where(row <= col, s, MASKED)
                else:
                    s = jnp.where(valid, s, MASKED)
                scores.append(s)
                high = jnp.max(s, axis=0, keepdims=True)
                top = high if top is None else jnp.maximum(top, high)
            shift = top * (SCALE * LOG2E)
            total = None
            mixed = None
            for b in range(blocks):
                w = jnp.exp2(scores[b] * (SCALE * LOG2E) - shift)
                part_sum = jnp.sum(w, axis=0, keepdims=True)
                total = part_sum if total is None else total + part_sum
                o = jnp.dot(
                    v_ext[g, :, pl.ds(pl.multiple_of(first + b * TILE, TILE), TILE)], w.astype(jnp.bfloat16),
                    preferred_element_type=jnp.float32,
                )
                mixed = o if mixed is None else mixed + o
            result = (mixed / total).astype(jnp.bfloat16)
            for i in range(groups):
                ctx[z, pl.ds((g * groups + i) * size, size), pl.ds(first, TILE)] = result[:, i * TILE : (i + 1) * TILE]

        @pl.when(z + 1 < n_head)
        def _():
            ctx_up(z, g).start()

        @pl.when(z >= 1)
        def _():
            ctx_down(z, g).start()

    tile = next(t for t in range(256, 0, -16) if feats % t == 0)

    def project(s, g, n=1):
        last = s == n_head - 1 and g + n == kv_heads
        r = order(s)
        if s > 0:
            @pl.when(jnp.logical_not(inner))
            def _():
                for i in range(n):
                    ctx_up(r, g + i).wait_recv()

        block = ctx[r, pl.ds(g * pair, n * pair), :]
        for j in range(sub):
            @pl.loop(0, feats // tile)
            def _(t):
                at = pl.ds(pl.multiple_of(t * tile, tile), tile)
                w = jnp.concatenate([w_all[g * groups + i, r, j, at, :] for i in range(n * groups)], 1)
                got = jnp.dot(w, block, preferred_element_type=jnp.float32)
                if s > 0 or g > 0:
                    got = got + acc[j, at, :]
                acc[j, at, :] = got
                if last:
                    squares[0] += jnp.sum((got * got).reshape(tile // 8, 8, rows), axis=0)

    loads = [pltpu.make_async_copy(src, dst, load_sem.at[i]) for i, (src, dst) in enumerate((
        (pos_hbm, pos_ref), (rate_hbm, rate_ref), (k_hbm, k_raw), (v_hbm, v_raw),
        (w_hbm, w_ref), (q_hbm, q_raw), (gain_hbm, gain_ref), (res_hbm, res_ref),
    ))]
    barrier = pltpu.get_barrier_semaphore()
    for d in range(1, n_seq):
        pl.semaphore_signal(barrier, inc=1, device_id=(lax.rem(me + d, n_seq), z), device_id_type=MESH)
    for d in range(1, n_head):
        pl.semaphore_signal(barrier, inc=1, device_id=(me, lax.rem(z + d, n_head)), device_id_type=MESH)
    for load in loads:
        load.start()

    def turned(x):
        x = jnp.swapaxes(x.astype(jnp.float32), 0, 1)
        return (x * cosine[None] + pltpu.roll(x, size // 2, 2) * sine[None]).astype(jnp.bfloat16)

    part = rows // 4
    for load in loads[:2]:
        load.wait()
    tokens = pos_ref[...].reshape(1, rows).astype(jnp.float32)
    early = lax.broadcasted_iota(jnp.int32, (size, size), 1) < size // 2
    for t in range(0, rows, size):
        angle = jnp.broadcast_to(tokens[:, t : t + size], (size, size)).T * rate_ref[...]
        cos_ref[t : t + size, :] = jnp.cos(angle)
        sine = jnp.sin(angle)
        sin_ref[t : t + size, :] = jnp.where(early, -sine, sine)
    loads[4].wait()
    pl.semaphore_wait(barrier, n_seq + n_head - 2)

    @pl.when(me // sub == z)
    def _():
        own_copy().start()

    @pl.when(me // sub != z)
    def _():
        own_climb().start()

    for word in LAUNCH:
        if word[0] != "H":
            scatter(others[int(word[1])])
    for load in loads[2:4]:
        load.wait()
    for t in range(0, rows, part):
        cosine, sine = cos_ref[t : t + part, :], sin_ref[t : t + part, :]
        k_ext[:, span + t : span + t + part, :] = turned(k_raw[t : t + part])
    for g in range(kv_heads):
        v_ext[g, :, span : span + rows] = v_raw[:, g, :].T
    for g in range(kv_heads):
        start_halo(g)
    squares[0] = jnp.zeros((8, rows), jnp.float32)
    loads[5].wait()
    for t in range(0, rows, part):
        cosine, sine = cos_ref[t : t + part, :], sin_ref[t : t + part, :]
        q_ref[:, t : t + part, :] = turned(q_raw[t : t + part])
    for dist in range(1, reach + 1):
        @pl.when(me < dist)
        def _():
            at = pl.ds(span - dist * rows, rows)
            k_ext[:, at, :] = jnp.zeros((kv_heads, rows, size), jnp.bfloat16)
            v_ext[:, :, at] = jnp.zeros((kv_heads, size, rows), jnp.bfloat16)
    loads[6].wait()
    gain_row = gain_ref[...].reshape(1, gain_ref.shape[0])
    for first in range(0, gain_ref.shape[0], LANES):
        count = min(LANES, gain_ref.shape[0] - first)
        gain_col[first : first + count, :] = jnp.broadcast_to(gain_row[:, first : first + count], (LANES, count)).T

    def take(n):
        take_piece(others[n])

    steps = {"T": take, "A": attend, "C": send_unit, "X": take_across, "Y": take_along, "D": take_corner,
             "S": take_relayed, "R": arrive, "P": project}
    for word in PLAN:
        steps[word[0]](*[int(c) for c in word[1:]])

    def sq(d, target):
        return remote(squares.at[0], squares.at[d], sq_send.at[d - 1], sq_recv.at[d - 1], (me, target))

    for d in range(1, n_head):
        sq(d, lax.rem(z + d, n_head)).start()
    for g in range(kv_heads):
        for dist in range(1, reach + 1):
            leaves = me + dist < n_seq
            if dist == 2:
                leaves = jnp.logical_and(even, leaves)

            @pl.when(leaves)
            def _():
                halo(dist, g, 0, me).wait_send()
                halo(dist, g, 1, me).wait_send()

        @pl.when(jnp.logical_and(even, me >= 1))
        def _():
            passed_on(g, 0).wait_send()
            passed_on(g, 1).wait_send()
    for target in others:
        piece(me, target, False).wait_send()
        source = target

        @pl.when(source // sub != z)
        def _():
            climb(source).wait_send()

    @pl.when(me // sub != z)
    def _():
        own_climb().wait_send()
    for s in range(n_head):
        for way in range(2):
            unit(me, s, unit_send.at[way, s], me).wait_send()
        unit(me, s, forward_send.at[s], me).wait_send()
        for way in range(4):
            unit(me, s, relay_send.at[way, s], me).wait_send()
    for g in range(kv_heads):
        for r in range(n_head):
            @pl.when(jnp.logical_and(r <= z, z + 1 < n_head))
            def _():
                ctx_up(r, g).wait_send()

            @pl.when(jnp.logical_and(r >= z, z >= 1))
            def _():
                ctx_down(r, g).wait_send()
    for d in range(1, n_head):
        sq(d, z).wait_recv()
    loads[7].wait()
    whole = jnp.sum(jnp.sum(squares[...], axis=0), axis=0, keepdims=True)
    inverse = lax.rsqrt(whole / (n_head * sub * feats) + EPS)
    for j in range(sub):
        at = pl.ds(j * feats, feats)
        gain = jnp.concatenate([gain_col[at, :]] * (rows // LANES), 1)
        out_ref[at, :] = (
            res_ref[at, :].astype(jnp.float32) + gain * (acc[j] * inverse)
        ).astype(jnp.bfloat16)

    for d in range(1, n_head):
        sq(d, z).wait_send()


def fits(rows, heads_rows, kv_heads, groups, feats, n_seq, n_head):
    return (
        n_seq == 8
        and n_head in (2, 4)
        and groups == 2
        and heads_rows == n_seq * LANES
        and rows % TILE == 0
        and VISIBLE_SPAN == 2 * rows
        and kv_heads * groups == n_seq
        and feats % 16 == 0
    )


def fused(positions, queries, keys, values, out_weight, post_gain, residual):
    n_seq, n_head = lax.axis_size("seq"), lax.axis_size("head")
    rows, kv_heads, size = keys.shape
    groups = queries.shape[1] // kv_heads
    feats = out_weight.shape[1]
    width = residual.shape[1]
    sub = n_seq // n_head
    reach = VISIBLE_SPAN // rows
    half = size // 2
    inverse = 10000.0 ** (-2.0 * jnp.arange(half, dtype=jnp.float32) / size)
    rate = jnp.concatenate([inverse, inverse])[None, :]
    bf16, f32 = jnp.bfloat16, jnp.float32
    dma = pltpu.SemaphoreType.DMA
    spec = pl.BlockSpec(memory_space=pltpu.VMEM)
    out = pl.pallas_call(
        functools.partial(layer_kernel, n_seq, n_head, kv_heads, groups, reach),
        out_shape=jax.ShapeDtypeStruct((width, rows), bf16),
        in_specs=[pl.BlockSpec(memory_space=pltpu.MemorySpace.HBM)] * 8,
        out_specs=spec,
        scratch_shapes=[
            pltpu.VMEM(queries.shape, bf16), pltpu.VMEM(keys.shape, bf16), pltpu.VMEM(keys.shape, bf16),
            pltpu.VMEM((rows,), jnp.int32), pltpu.VMEM((1, size), f32), pltpu.VMEM(out_weight.shape[::-1], bf16),
            pltpu.VMEM((width,), f32), pltpu.VMEM((width, rows), bf16), dma((8,)),
            pltpu.VMEM((rows, size), f32), pltpu.VMEM((rows, size), f32),
            pltpu.VMEM((kv_heads * groups, rows, size), bf16),
            pltpu.VMEM((width, LANES), f32),
            pltpu.VMEM((kv_heads, (reach + 1) * rows, size), bf16),
            pltpu.VMEM((kv_heads, size, (reach + 1) * rows), bf16),
            pltpu.VMEM((n_seq, feats, LANES), bf16),
            pltpu.VMEM((n_seq, n_head, sub, feats, LANES), bf16),
            pltpu.VMEM((n_head, kv_heads * groups * size, rows), bf16),
            pltpu.VMEM((sub, feats, rows), f32),
            pltpu.VMEM((n_head, 8, rows), f32),
            dma((reach, kv_heads, 2)), dma((reach, kv_heads, 2)), dma((kv_heads, 2)),
            dma((n_seq,)), dma((n_seq,)), dma, dma((n_seq,)), dma((n_head, sub)),
            dma((2, n_head)), dma((n_head,)), dma((4, n_head)), dma((n_seq, n_head)),
            dma((n_head, kv_heads)), dma((n_head, kv_heads)), dma((n_head, kv_heads)),
            dma((n_head,)), dma((n_head,)),
        ],
        compiler_params=pltpu.CompilerParams(has_side_effects=True, collective_id=0, vmem_limit_bytes=44 * 1024 * 1024),
    )(*[pltpu.with_memory_space_constraint(x, pltpu.MemorySpace.HBM) for x in (queries, keys, values, positions, rate, out_weight.T, post_gain, residual.T)])
    return out.T


def general(positions, queries, keys, values, out_weight, post_gain, residual):
    rows = queries.shape[0]
    kv_heads = keys.shape[1]
    query_groups = QUERY_HEADS // KEY_VALUE_HEADS
    q_rot = rotate(queries, positions)
    stacked = jnp.stack([rotate(keys, positions), values], 0)
    reach = (VISIBLE_SPAN + rows - 2) // rows
    pieces = []
    carried = stacked
    for hop in range(reach):
        carried = passed_along(carried, "seq", 1)
        pieces.insert(0, carried)
    extended = jnp.concatenate(pieces + [stacked], axis=1)
    extra = extended.shape[1] - rows
    anchor = lax.axis_index("seq") * rows
    tile_rows = q_rot.reshape(rows, kv_heads, query_groups, -1)
    scores = jnp.einsum("qhgd,khd->hgqk", tile_rows, extended[0], preferred_element_type=jnp.float32) * SCALE
    query_index = anchor + jnp.arange(rows, dtype=jnp.int32)
    key_index = anchor - extra + jnp.arange(extra + rows, dtype=jnp.int32)
    gap = query_index[:, None] - key_index[None, :]
    allowed = (gap >= 0) & (gap < VISIBLE_SPAN) & (key_index[None, :] >= 0)
    scores = jnp.where(allowed, scores, MASKED)
    top = jnp.max(scores, axis=-1, keepdims=True)
    weights = jnp.exp(scores - top)
    probs = (weights / jnp.sum(weights, axis=-1, keepdims=True)).astype(jnp.bfloat16)
    context = jnp.einsum("hgqk,khd->qhgd", probs, extended[1], preferred_element_type=jnp.float32)
    context = context.astype(jnp.bfloat16).reshape(rows, -1)
    partial_value = jnp.dot(
        context,
        lax.all_gather(out_weight, "seq", axis=1, tiled=True),
        preferred_element_type=jnp.float32,
    )
    attended = lax.psum_scatter(
        partial_value.astype(jnp.bfloat16), "head", scatter_dimension=1, tiled=True
    ).astype(jnp.float32)
    squares = lax.psum(jnp.sum(attended * attended, axis=1), "head")
    scaled = attended * lax.rsqrt(squares / D + EPS)[:, None]
    result = residual.astype(jnp.float32) + post_gain[None, :] * scaled
    return result.astype(jnp.bfloat16)


def on_device(positions, queries, keys, values, out_weight, post_gain, residual):
    n_seq, n_head = lax.axis_size("seq"), lax.axis_size("head")
    rows, kv_heads, _ = keys.shape
    body = fused if fits(rows, out_weight.shape[0], kv_heads, queries.shape[1] // kv_heads, out_weight.shape[1], n_seq, n_head) else general
    return body(positions, queries, keys, values, out_weight, post_gain, residual)


def solution(mesh):
    return jax.shard_map(
        on_device,
        mesh=mesh,
        in_specs=(
            P("seq"),
            P("seq", "head", None),
            P("seq", "head", None),
            P("seq", "head", None),
            P("head", "seq"),
            P("head"),
            P("seq", "head"),
        ),
        out_specs=P("seq", "head"),
        check_vma=False,
    )
```

```python
import functools

import jax
import jax.numpy as jnp
from jax import lax
from jax.experimental import pallas as pl
from jax.experimental.pallas import tpu as pltpu
from jax.sharding import PartitionSpec as P

D = 5376
QUERY_HEADS = 32
KEY_VALUE_HEADS = 16
VISIBLE_SPAN = 1024


EPS = 1e-06
SCALE = 168.0 ** (-0.5)
LOG2E = 1.4426950408889634
MASKED = -1e30
TILE = 256
LANES = 128
MESH = pl.DeviceIdType.MESH
LAUNCH = (
    "Z4", "Z0", "Z1", "Z2", "Z3", "Z5", "Z6", "H0", "H1", "H2", "H3",
)
PLAN = (
    "T6", "T4", "T0", "T1", "T2", "T3", "T5", "C0", "A0", "A1", "A2", "A3",
    "C1", "C2", "C3", "R10", "R11", "R12", "R13", "R20", "R21", "X0", "Y0", "D0",
    "S0", "R22", "R23", "P004", "R30", "R31", "R32", "X1", "Y1", "D1", "S1", "P104",
    "R33", "X2", "Y2", "D2", "S2", "P204", "X3", "Y3", "D3", "S3", "P303", "P33",
)
DIRECT = (0, 1, 2, 3, )


def passed_along(value, axis, steps):
    count = lax.axis_size(axis)
    initial, last = (max(0, -steps), min(count, count - steps))
    return lax.ppermute(value, axis, [(source, source + steps) for source in range(initial, last)])


def rotate(x, positions):
    half = x.shape[-1] // 2
    inverse = 10000.0 ** (-2.0 * jnp.arange(half, dtype=jnp.float32) / x.shape[-1])
    angle = positions.astype(jnp.float32)[:, None] * inverse[None, :]
    cosine = jnp.concatenate([jnp.cos(angle), jnp.cos(angle)], -1)[:, None, :]
    sine = jnp.concatenate([jnp.sin(angle), jnp.sin(angle)], -1)[:, None, :]
    source = x.astype(jnp.float32)
    turned = jnp.concatenate([-source[..., half:], source[..., :half]], -1)
    return (source * cosine + turned * sine).astype(jnp.bfloat16)


def layer_kernel(
    n_seq, n_head, kv_heads, groups, reach,
    q_hbm, k_hbm, v_hbm, pos_hbm, rate_hbm, w_hbm, gain_hbm, res_hbm, out_ref,
    q_raw, k_raw, v_raw, pos_ref, rate_ref, w_ref, gain_ref, res_ref, load_sem,
    cos_ref, sin_ref,
    q_ref, gain_col, k_ext, v_ext, stage, w_all, ctx, acc, squares,
    halo_send, halo_recv, pass_send, a_send, a_recv, own_sem, c_send, c_recv,
    unit_send, forward_send, relay_send, unit_recv,
    up_send, down_send, ctx_recv, sq_send, sq_recv,
):
    me = lax.axis_index("seq")
    z = lax.axis_index("head")
    rows = k_raw.shape[0]
    size = k_raw.shape[2]
    feats = w_ref.shape[0]
    sub = n_seq // n_head
    span = reach * rows
    core = lax.rem(me, 2)
    chip = me // 2
    even = core == 0
    sibling = me + 1 - 2 * core
    across = me + 2 - 4 * lax.rem(chip, 2)
    along = me + 4 - 8 * (chip // 2)
    corner = across + along - me
    pair = groups * size

    def remote(src, dst, send, recv, device):
        return pltpu.make_async_remote_copy(
            src_ref=src, dst_ref=dst, send_sem=send, recv_sem=recv,
            device_id=device, device_id_type=MESH,
        )

    def order(s):
        low = z < n_head // 2
        near = jnp.where(low, z, n_head - 1 - z)
        at = near if s == 0 else (1 - near if s == 1 else s)
        return jnp.where(low, at, n_head - 1 - at)

    def halo(dist, g, kv, target):
        at, own = pl.ds(span - dist * rows, rows), pl.ds(span, rows)
        if kv == 0:
            src, dst = k_ext.at[g, own, :], k_ext.at[g, at, :]
        else:
            src, dst = v_ext.at[g, :, own], v_ext.at[g, :, at]
        return remote(src, dst, halo_send.at[dist - 1, g, kv], halo_recv.at[dist - 1, g, kv], (target, z))

    def passed_on(g, kv):
        near, far = pl.ds(span - rows, rows), pl.ds(span - 2 * rows, rows)
        if kv == 0:
            src, dst = k_ext.at[g, near, :], k_ext.at[g, far, :]
        else:
            src, dst = v_ext.at[g, :, near], v_ext.at[g, :, far]
        return remote(src, dst, pass_send.at[g, kv], halo_recv.at[1, g, kv], (me + 1, z))

    def start_halo(g):
        @pl.when(me + 1 < n_seq)
        def _():
            halo(1, g, 0, me + 1).start()
            halo(1, g, 1, me + 1).start()

        @pl.when(jnp.logical_and(even, me + 2 < n_seq))
        def _():
            halo(2, g, 0, me + 2).start()
            halo(2, g, 1, me + 2).start()

    def columns(target):
        return w_ref.at[:, pl.ds(pl.multiple_of(target * LANES, LANES), LANES)]

    def piece(source, target, direct):
        dst = w_all.at[target, z, lax.rem(source, sub)] if direct else stage.at[source]
        return remote(columns(target), dst, a_send.at[target], a_recv.at[source], (target, z))

    def scatter(target):
        @pl.when(me // sub == z)
        def _():
            piece(me, target, True).start()

        @pl.when(me // sub != z)
        def _():
            piece(me, target, False).start()

    def own_copy():
        return pltpu.make_async_copy(columns(me), w_all.at[me, z, lax.rem(me, sub)], own_sem)

    def own_climb():
        return remote(
            columns(me), w_all.at[me, z, lax.rem(me, sub)],
            c_send.at[me], c_recv.at[z, lax.rem(me, sub)], (me, me // sub),
        )

    def climb(source):
        return remote(
            stage.at[source], w_all.at[me, z, lax.rem(source, sub)],
            c_send.at[source], c_recv.at[z, lax.rem(source, sub)], (me, source // sub),
        )

    def take_piece(source):
        piece(source, me, False).wait_recv()

        @pl.when(source // sub != z)
        def _():
            climb(source).start()

    others = (across, along, across + 1 - 2 * core, along + 1 - 2 * core, corner, corner + 1 - 2 * core, sibling)

    def unit(owner, r, send, target):
        return remote(w_all.at[owner, r], w_all.at[owner, r], send, unit_recv.at[owner, r], (target, z))

    def send_unit(s):
        r = order(s)
        if s == 0:
            @pl.when(me // sub == z)
            def _():
                own_copy().wait()

        else:
            for j in range(sub):
                remote(stage.at[0], w_all.at[me, r, j], c_send.at[0], c_recv.at[r, j], (me, r)).wait_recv()
        unit(me, r, unit_send.at[0, s], across).start()
        unit(me, r, unit_send.at[1, s], along).start()
        if s in DIRECT:
            unit(me, r, forward_send.at[s], corner).start()
        unit(me, r, relay_send.at[0, s], sibling).start()

    def take_across(s):
        r = order(s)
        unit(across, r, unit_send.at[0, s], me).wait_recv()

        @pl.when(jnp.logical_and(even, s not in DIRECT))
        def _():
            unit(across, r, forward_send.at[s], along).start()

        unit(across, r, relay_send.at[1, s], sibling).start()

    def take_along(s):
        r = order(s)
        unit(along, r, unit_send.at[0, s], me).wait_recv()

        @pl.when(jnp.logical_and(jnp.logical_not(even), s not in DIRECT))
        def _():
            unit(along, r, forward_send.at[s], across).start()

        unit(along, r, relay_send.at[2, s], sibling).start()

    def take_corner(s):
        r = order(s)
        unit(corner, r, unit_send.at[0, s], me).wait_recv()
        unit(corner, r, relay_send.at[3, s], sibling).start()

    def take_relayed(s):
        r = order(s)
        for owner in (me, across, along, corner):
            unit(owner + 1 - 2 * core, r, unit_send.at[0, s], me).wait_recv()

    def chunk(r, g):
        return ctx.at[r, pl.ds(g * pair, pair), :]

    def ctx_up(r, g):
        return remote(chunk(r, g), chunk(r, g), up_send.at[r, g], ctx_recv.at[r, g], (me, z + 1))

    def ctx_down(r, g):
        return remote(chunk(r, g), chunk(r, g), down_send.at[r, g], ctx_recv.at[r, g], (me, z - 1))

    inner = jnp.logical_and(z >= 1, z + 1 < n_head)

    def arrive(s, g):
        r = order(s)

        @pl.when(inner)
        def _():
            ctx_up(r, g).wait_recv()

        @pl.when(jnp.logical_and(inner, r < z))
        def _():
            ctx_up(r, g).start()

        @pl.when(jnp.logical_and(inner, r > z))
        def _():
            ctx_down(r, g).start()

    blocks = span // TILE + 1

    def attend(g):
        for dist in range(1, reach + 1):
            @pl.when(me >= dist)
            def _():
                halo(dist, g, 0, me).wait_recv()
                halo(dist, g, 1, me).wait_recv()
                if dist == 1:
                    @pl.when(even)
                    def _():
                        passed_on(g, 0).start()
                        passed_on(g, 1).start()

        @pl.loop(0, rows // TILE)
        def _(t):
            first = pl.multiple_of(t * TILE, TILE)
            q = jnp.concatenate([q_ref[g * groups + i, pl.ds(first, TILE), :] for i in range(groups)], 0)
            row = lax.broadcasted_iota(jnp.int32, (TILE, groups * TILE), 0)
            col = lax.rem(lax.broadcasted_iota(jnp.int32, (TILE, groups * TILE), 1), TILE)
            scores = []
            top = None
            for b in range(blocks):
                s = lax.dot_general(
                    k_ext[g, pl.ds(first + b * TILE, TILE), :], q,
                    (((1,), (1,)), ((), ())), preferred_element_type=jnp.float32,
                )
                valid = me * rows + first + b * TILE - span >= 0
                if b == 0:
                    s = jnp.where(jnp.logical_and(row > col, valid), s, MASKED)
                elif b == blocks - 1:
                    s = jnp.where(row <= col, s, MASKED)
                else:
                    s = jnp.where(valid, s, MASKED)
                scores.append(s)
                high = jnp.max(s, axis=0, keepdims=True)
                top = high if top is None else jnp.maximum(top, high)
            shift = top * (SCALE * LOG2E)
            total = None
            mixed = None
            for b in range(blocks):
                w = jnp.exp2(scores[b] * (SCALE * LOG2E) - shift)
                part_sum = jnp.sum(w, axis=0, keepdims=True)
                total = part_sum if total is None else total + part_sum
                o = jnp.dot(
                    v_ext[g, :, pl.ds(pl.multiple_of(first + b * TILE, TILE), TILE)], w.astype(jnp.bfloat16),
                    preferred_element_type=jnp.float32,
                )
                mixed = o if mixed is None else mixed + o
            result = (mixed / total).astype(jnp.bfloat16)
            for i in range(groups):
                ctx[z, pl.ds((g * groups + i) * size, size), pl.ds(first, TILE)] = result[:, i * TILE : (i + 1) * TILE]

        @pl.when(z + 1 < n_head)
        def _():
            ctx_up(z, g).start()

        @pl.when(z >= 1)
        def _():
            ctx_down(z, g).start()

    tile = next(t for t in range(feats, 0, -16) if feats % t == 0)

    def project(s, g, n=1):
        last = s == n_head - 1 and g + n == kv_heads
        r = order(s)
        if s > 0:
            @pl.when(jnp.logical_not(inner))
            def _():
                for i in range(n):
                    ctx_up(r, g + i).wait_recv()

        block = ctx[r, pl.ds(g * pair, n * pair), :]
        for j in range(sub):
            @pl.loop(0, feats // tile)
            def _(t):
                at = pl.ds(pl.multiple_of(t * tile, tile), tile)
                w = jnp.concatenate([w_all[g * groups + i, r, j, at, :] for i in range(n * groups)], 1)
                got = jnp.dot(w, block, preferred_element_type=jnp.float32)
                if s > 0 or g > 0:
                    got = got + acc[j, at, :]
                acc[j, at, :] = got
                if last:
                    squares[0] += jnp.sum((got * got).reshape(tile // 8, 8, rows), axis=0)

    loads = [pltpu.make_async_copy(src, dst, load_sem.at[i]) for i, (src, dst) in enumerate((
        (pos_hbm, pos_ref), (rate_hbm, rate_ref), (k_hbm, k_raw), (v_hbm, v_raw),
        (w_hbm, w_ref), (q_hbm, q_raw), (gain_hbm, gain_ref), (res_hbm, res_ref),
    ))]
    barrier = pltpu.get_barrier_semaphore()
    for d in range(1, n_seq):
        pl.semaphore_signal(barrier, inc=1, device_id=(lax.rem(me + d, n_seq), z), device_id_type=MESH)
    for d in range(1, n_head):
        pl.semaphore_signal(barrier, inc=1, device_id=(me, lax.rem(z + d, n_head)), device_id_type=MESH)
    for load in loads:
        load.start()

    def turned(x):
        x = jnp.swapaxes(x.astype(jnp.float32), 0, 1)
        return (x * cosine[None] + pltpu.roll(x, size // 2, 2) * sine[None]).astype(jnp.bfloat16)

    part = rows // 4
    for load in loads[:2]:
        load.wait()
    tokens = pos_ref[...].reshape(1, rows).astype(jnp.float32)
    early = lax.broadcasted_iota(jnp.int32, (size, size), 1) < size // 2
    for t in range(0, rows, size):
        angle = jnp.broadcast_to(tokens[:, t : t + size], (size, size)).T * rate_ref[...]
        cos_ref[t : t + size, :] = jnp.cos(angle)
        sine = jnp.sin(angle)
        sin_ref[t : t + size, :] = jnp.where(early, -sine, sine)
    loads[4].wait()
    pl.semaphore_wait(barrier, n_seq + n_head - 2)

    @pl.when(me // sub == z)
    def _():
        own_copy().start()

    @pl.when(me // sub != z)
    def _():
        own_climb().start()

    for word in LAUNCH:
        if word[0] != "H":
            scatter(others[int(word[1])])
    for load in loads[2:4]:
        load.wait()
    for t in range(0, rows, part):
        cosine, sine = cos_ref[t : t + part, :], sin_ref[t : t + part, :]
        k_ext[:, span + t : span + t + part, :] = turned(k_raw[t : t + part])
    for g in range(kv_heads):
        v_ext[g, :, span : span + rows] = v_raw[:, g, :].T
    for g in range(kv_heads):
        start_halo(g)
    squares[0] = jnp.zeros((8, rows), jnp.float32)
    loads[5].wait()
    for t in range(0, rows, part):
        cosine, sine = cos_ref[t : t + part, :], sin_ref[t : t + part, :]
        q_ref[:, t : t + part, :] = turned(q_raw[t : t + part])
    for dist in range(1, reach + 1):
        @pl.when(me < dist)
        def _():
            at = pl.ds(span - dist * rows, rows)
            k_ext[:, at, :] = jnp.zeros((kv_heads, rows, size), jnp.bfloat16)
            v_ext[:, :, at] = jnp.zeros((kv_heads, size, rows), jnp.bfloat16)
    loads[6].wait()
    gain_row = gain_ref[...].reshape(1, gain_ref.shape[0])
    for first in range(0, gain_ref.shape[0], LANES):
        count = min(LANES, gain_ref.shape[0] - first)
        gain_col[first : first + count, :] = jnp.broadcast_to(gain_row[:, first : first + count], (LANES, count)).T

    def take(n):
        take_piece(others[n])

    steps = {"T": take, "A": attend, "C": send_unit, "X": take_across, "Y": take_along, "D": take_corner,
             "S": take_relayed, "R": arrive, "P": project}
    for word in PLAN:
        steps[word[0]](*[int(c) for c in word[1:]])

    def sq(d, target):
        return remote(squares.at[0], squares.at[d], sq_send.at[d - 1], sq_recv.at[d - 1], (me, target))

    for d in range(1, n_head):
        sq(d, lax.rem(z + d, n_head)).start()
    for g in range(kv_heads):
        for dist in range(1, reach + 1):
            leaves = me + dist < n_seq
            if dist == 2:
                leaves = jnp.logical_and(even, leaves)

            @pl.when(leaves)
            def _():
                halo(dist, g, 0, me).wait_send()
                halo(dist, g, 1, me).wait_send()

        @pl.when(jnp.logical_and(even, me >= 1))
        def _():
            passed_on(g, 0).wait_send()
            passed_on(g, 1).wait_send()
    for target in others:
        piece(me, target, False).wait_send()
        source = target

        @pl.when(source // sub != z)
        def _():
            climb(source).wait_send()

    @pl.when(me // sub != z)
    def _():
        own_climb().wait_send()
    for s in range(n_head):
        for way in range(2):
            unit(me, s, unit_send.at[way, s], me).wait_send()
        unit(me, s, forward_send.at[s], me).wait_send()
        for way in range(4):
            unit(me, s, relay_send.at[way, s], me).wait_send()
    for g in range(kv_heads):
        for r in range(n_head):
            @pl.when(jnp.logical_and(r <= z, z + 1 < n_head))
            def _():
                ctx_up(r, g).wait_send()

            @pl.when(jnp.logical_and(r >= z, z >= 1))
            def _():
                ctx_down(r, g).wait_send()
    for d in range(1, n_head):
        sq(d, z).wait_recv()
    loads[7].wait()
    whole = jnp.sum(jnp.sum(squares[...], axis=0), axis=0, keepdims=True)
    inverse = lax.rsqrt(whole / (n_head * sub * feats) + EPS)
    for j in range(sub):
        at = pl.ds(j * feats, feats)
        gain = jnp.concatenate([gain_col[at, :]] * (rows // LANES), 1)
        out_ref[at, :] = (
            res_ref[at, :].astype(jnp.float32) + gain * (acc[j] * inverse)
        ).astype(jnp.bfloat16)

    for d in range(1, n_head):
        sq(d, z).wait_send()


def fits(rows, heads_rows, kv_heads, groups, feats, n_seq, n_head):
    return (
        n_seq == 8
        and n_head in (2, 4)
        and groups == 2
        and heads_rows == n_seq * LANES
        and rows % TILE == 0
        and VISIBLE_SPAN == 2 * rows
        and kv_heads * groups == n_seq
        and feats % 16 == 0
    )


def fused(positions, queries, keys, values, out_weight, post_gain, residual):
    n_seq, n_head = lax.axis_size("seq"), lax.axis_size("head")
    rows, kv_heads, size = keys.shape
    groups = queries.shape[1] // kv_heads
    feats = out_weight.shape[1]
    width = residual.shape[1]
    sub = n_seq // n_head
    reach = VISIBLE_SPAN // rows
    half = size // 2
    inverse = 10000.0 ** (-2.0 * jnp.arange(half, dtype=jnp.float32) / size)
    rate = jnp.concatenate([inverse, inverse])[None, :]
    bf16, f32 = jnp.bfloat16, jnp.float32
    dma = pltpu.SemaphoreType.DMA
    spec = pl.BlockSpec(memory_space=pltpu.VMEM)
    out = pl.pallas_call(
        functools.partial(layer_kernel, n_seq, n_head, kv_heads, groups, reach),
        out_shape=jax.ShapeDtypeStruct((width, rows), bf16),
        in_specs=[pl.BlockSpec(memory_space=pltpu.MemorySpace.HBM)] * 8,
        out_specs=spec,
        scratch_shapes=[
            pltpu.VMEM(queries.shape, bf16), pltpu.VMEM(keys.shape, bf16), pltpu.VMEM(keys.shape, bf16),
            pltpu.VMEM((rows,), jnp.int32), pltpu.VMEM((1, size), f32), pltpu.VMEM(out_weight.shape[::-1], bf16),
            pltpu.VMEM((width,), f32), pltpu.VMEM((width, rows), bf16), dma((8,)),
            pltpu.VMEM((rows, size), f32), pltpu.VMEM((rows, size), f32),
            pltpu.VMEM((kv_heads * groups, rows, size), bf16),
            pltpu.VMEM((width, LANES), f32),
            pltpu.VMEM((kv_heads, (reach + 1) * rows, size), bf16),
            pltpu.VMEM((kv_heads, size, (reach + 1) * rows), bf16),
            pltpu.VMEM((n_seq, feats, LANES), bf16),
            pltpu.VMEM((n_seq, n_head, sub, feats, LANES), bf16),
            pltpu.VMEM((n_head, kv_heads * groups * size, rows), bf16),
            pltpu.VMEM((sub, feats, rows), f32),
            pltpu.VMEM((n_head, 8, rows), f32),
            dma((reach, kv_heads, 2)), dma((reach, kv_heads, 2)), dma((kv_heads, 2)),
            dma((n_seq,)), dma((n_seq,)), dma, dma((n_seq,)), dma((n_head, sub)),
            dma((2, n_head)), dma((n_head,)), dma((4, n_head)), dma((n_seq, n_head)),
            dma((n_head, kv_heads)), dma((n_head, kv_heads)), dma((n_head, kv_heads)),
            dma((n_head,)), dma((n_head,)),
        ],
        compiler_params=pltpu.CompilerParams(has_side_effects=True, collective_id=0, vmem_limit_bytes=44 * 1024 * 1024),
    )(*[pltpu.with_memory_space_constraint(x, pltpu.MemorySpace.HBM) for x in (queries, keys, values, positions, rate, out_weight.T, post_gain, residual.T)])
    return out.T


def general(positions, queries, keys, values, out_weight, post_gain, residual):
    rows = queries.shape[0]
    kv_heads = keys.shape[1]
    query_groups = QUERY_HEADS // KEY_VALUE_HEADS
    q_rot = rotate(queries, positions)
    stacked = jnp.stack([rotate(keys, positions), values], 0)
    reach = (VISIBLE_SPAN + rows - 2) // rows
    pieces = []
    carried = stacked
    for hop in range(reach):
        carried = passed_along(carried, "seq", 1)
        pieces.insert(0, carried)
    extended = jnp.concatenate(pieces + [stacked], axis=1)
    extra = extended.shape[1] - rows
    anchor = lax.axis_index("seq") * rows
    tile_rows = q_rot.reshape(rows, kv_heads, query_groups, -1)
    scores = jnp.einsum("qhgd,khd->hgqk", tile_rows, extended[0], preferred_element_type=jnp.float32) * SCALE
    query_index = anchor + jnp.arange(rows, dtype=jnp.int32)
    key_index = anchor - extra + jnp.arange(extra + rows, dtype=jnp.int32)
    gap = query_index[:, None] - key_index[None, :]
    allowed = (gap >= 0) & (gap < VISIBLE_SPAN) & (key_index[None, :] >= 0)
    scores = jnp.where(allowed, scores, MASKED)
    top = jnp.max(scores, axis=-1, keepdims=True)
    weights = jnp.exp(scores - top)
    probs = (weights / jnp.sum(weights, axis=-1, keepdims=True)).astype(jnp.bfloat16)
    context = jnp.einsum("hgqk,khd->qhgd", probs, extended[1], preferred_element_type=jnp.float32)
    context = context.astype(jnp.bfloat16).reshape(rows, -1)
    partial_value = jnp.dot(
        context,
        lax.all_gather(out_weight, "seq", axis=1, tiled=True),
        preferred_element_type=jnp.float32,
    )
    attended = lax.psum_scatter(
        partial_value.astype(jnp.bfloat16), "head", scatter_dimension=1, tiled=True
    ).astype(jnp.float32)
    squares = lax.psum(jnp.sum(attended * attended, axis=1), "head")
    scaled = attended * lax.rsqrt(squares / D + EPS)[:, None]
    result = residual.astype(jnp.float32) + post_gain[None, :] * scaled
    return result.astype(jnp.bfloat16)


def on_device(positions, queries, keys, values, out_weight, post_gain, residual):
    n_seq, n_head = lax.axis_size("seq"), lax.axis_size("head")
    rows, kv_heads, _ = keys.shape
    body = fused if fits(rows, out_weight.shape[0], kv_heads, queries.shape[1] // kv_heads, out_weight.shape[1], n_seq, n_head) else general
    return body(positions, queries, keys, values, out_weight, post_gain, residual)


def solution(mesh):
    return jax.shard_map(
        on_device,
        mesh=mesh,
        in_specs=(
            P("seq"),
            P("seq", "head", None),
            P("seq", "head", None),
            P("seq", "head", None),
            P("head", "seq"),
            P("head"),
            P("seq", "head"),
        ),
        out_specs=P("seq", "head"),
        check_vma=False,
    )
```

```python
import functools

import jax
import jax.numpy as jnp
from jax import lax
from jax.experimental import pallas as pl
from jax.experimental.pallas import tpu as pltpu
from jax.sharding import PartitionSpec as P

D = 5376
QUERY_HEADS = 32
KEY_VALUE_HEADS = 16
VISIBLE_SPAN = 1024


EPS = 1e-06
SCALE = 168.0 ** (-0.5)
LOG2E = 1.4426950408889634
MASKED = -1e30
TILE = 256
LANES = 128
MESH = pl.DeviceIdType.MESH
LAUNCH = (
    "Z4", "Z0", "Z1", "Z2", "Z3", "Z5", "Z6", "H0", "H1", "H2", "H3",
)
PLAN = (
    "T6", "T4", "T0", "T1", "T2", "T3", "T5", "C0", "A0", "A1", "A2", "A3",
    "C1", "C2", "C3", "R10", "R11", "R12", "R13", "R20", "R21", "X0", "Y0", "D0",
    "S0", "R22", "R23", "P004", "R30", "R31", "R32", "X1", "Y1", "D1", "S1", "P104",
    "R33", "X2", "Y2", "D2", "S2", "P204", "X3", "Y3", "D3", "S3", "P302", "P322",
)
DIRECT = (0, 1, 2, 3, )


def passed_along(value, axis, steps):
    count = lax.axis_size(axis)
    initial, last = (max(0, -steps), min(count, count - steps))
    return lax.ppermute(value, axis, [(source, source + steps) for source in range(initial, last)])


def rotate(x, positions):
    half = x.shape[-1] // 2
    inverse = 10000.0 ** (-2.0 * jnp.arange(half, dtype=jnp.float32) / x.shape[-1])
    angle = positions.astype(jnp.float32)[:, None] * inverse[None, :]
    cosine = jnp.concatenate([jnp.cos(angle), jnp.cos(angle)], -1)[:, None, :]
    sine = jnp.concatenate([jnp.sin(angle), jnp.sin(angle)], -1)[:, None, :]
    source = x.astype(jnp.float32)
    turned = jnp.concatenate([-source[..., half:], source[..., :half]], -1)
    return (source * cosine + turned * sine).astype(jnp.bfloat16)


def layer_kernel(
    n_seq, n_head, kv_heads, groups, reach,
    q_hbm, k_hbm, v_hbm, pos_hbm, rate_hbm, w_hbm, gain_hbm, res_hbm, out_ref,
    q_raw, k_raw, v_raw, pos_ref, rate_ref, w_ref, gain_ref, res_ref, load_sem,
    cos_ref, sin_ref,
    q_ref, gain_col, k_ext, v_ext, stage, w_all, ctx, acc, squares,
    halo_send, halo_recv, pass_send, a_send, a_recv, own_sem, c_send, c_recv,
    unit_send, forward_send, relay_send, unit_recv,
    up_send, down_send, ctx_recv, sq_send, sq_recv,
):
    me = lax.axis_index("seq")
    z = lax.axis_index("head")
    rows = k_raw.shape[0]
    size = k_raw.shape[2]
    feats = w_ref.shape[0]
    sub = n_seq // n_head
    span = reach * rows
    core = lax.rem(me, 2)
    chip = me // 2
    even = core == 0
    sibling = me + 1 - 2 * core
    across = me + 2 - 4 * lax.rem(chip, 2)
    along = me + 4 - 8 * (chip // 2)
    corner = across + along - me
    pair = groups * size

    def remote(src, dst, send, recv, device):
        return pltpu.make_async_remote_copy(
            src_ref=src, dst_ref=dst, send_sem=send, recv_sem=recv,
            device_id=device, device_id_type=MESH,
        )

    def order(s):
        low = z < n_head // 2
        near = jnp.where(low, z, n_head - 1 - z)
        at = near if s == 0 else (1 - near if s == 1 else s)
        return jnp.where(low, at, n_head - 1 - at)

    def halo(dist, g, kv, target):
        at, own = pl.ds(span - dist * rows, rows), pl.ds(span, rows)
        if kv == 0:
            src, dst = k_ext.at[g, own, :], k_ext.at[g, at, :]
        else:
            src, dst = v_ext.at[g, :, own], v_ext.at[g, :, at]
        return remote(src, dst, halo_send.at[dist - 1, g, kv], halo_recv.at[dist - 1, g, kv], (target, z))

    def passed_on(g, kv):
        near, far = pl.ds(span - rows, rows), pl.ds(span - 2 * rows, rows)
        if kv == 0:
            src, dst = k_ext.at[g, near, :], k_ext.at[g, far, :]
        else:
            src, dst = v_ext.at[g, :, near], v_ext.at[g, :, far]
        return remote(src, dst, pass_send.at[g, kv], halo_recv.at[1, g, kv], (me + 1, z))

    def start_halo(g):
        @pl.when(me + 1 < n_seq)
        def _():
            halo(1, g, 0, me + 1).start()
            halo(1, g, 1, me + 1).start()

        @pl.when(jnp.logical_and(even, me + 2 < n_seq))
        def _():
            halo(2, g, 0, me + 2).start()
            halo(2, g, 1, me + 2).start()

    def columns(target):
        return w_ref.at[:, pl.ds(pl.multiple_of(target * LANES, LANES), LANES)]

    def piece(source, target, direct):
        dst = w_all.at[target, z, lax.rem(source, sub)] if direct else stage.at[source]
        return remote(columns(target), dst, a_send.at[target], a_recv.at[source], (target, z))

    def scatter(target):
        @pl.when(me // sub == z)
        def _():
            piece(me, target, True).start()

        @pl.when(me // sub != z)
        def _():
            piece(me, target, False).start()

    def own_copy():
        return pltpu.make_async_copy(columns(me), w_all.at[me, z, lax.rem(me, sub)], own_sem)

    def own_climb():
        return remote(
            columns(me), w_all.at[me, z, lax.rem(me, sub)],
            c_send.at[me], c_recv.at[z, lax.rem(me, sub)], (me, me // sub),
        )

    def climb(source):
        return remote(
            stage.at[source], w_all.at[me, z, lax.rem(source, sub)],
            c_send.at[source], c_recv.at[z, lax.rem(source, sub)], (me, source // sub),
        )

    def take_piece(source):
        piece(source, me, False).wait_recv()

        @pl.when(source // sub != z)
        def _():
            climb(source).start()

    others = (across, along, across + 1 - 2 * core, along + 1 - 2 * core, corner, corner + 1 - 2 * core, sibling)

    def unit(owner, r, send, target):
        return remote(w_all.at[owner, r], w_all.at[owner, r], send, unit_recv.at[owner, r], (target, z))

    def send_unit(s):
        r = order(s)
        if s == 0:
            @pl.when(me // sub == z)
            def _():
                own_copy().wait()

        else:
            for j in range(sub):
                remote(stage.at[0], w_all.at[me, r, j], c_send.at[0], c_recv.at[r, j], (me, r)).wait_recv()
        unit(me, r, unit_send.at[0, s], across).start()
        unit(me, r, unit_send.at[1, s], along).start()
        if s in DIRECT:
            unit(me, r, forward_send.at[s], corner).start()
        unit(me, r, relay_send.at[0, s], sibling).start()

    def take_across(s):
        r = order(s)
        unit(across, r, unit_send.at[0, s], me).wait_recv()

        @pl.when(jnp.logical_and(even, s not in DIRECT))
        def _():
            unit(across, r, forward_send.at[s], along).start()

        unit(across, r, relay_send.at[1, s], sibling).start()

    def take_along(s):
        r = order(s)
        unit(along, r, unit_send.at[0, s], me).wait_recv()

        @pl.when(jnp.logical_and(jnp.logical_not(even), s not in DIRECT))
        def _():
            unit(along, r, forward_send.at[s], across).start()

        unit(along, r, relay_send.at[2, s], sibling).start()

    def take_corner(s):
        r = order(s)
        unit(corner, r, unit_send.at[0, s], me).wait_recv()
        unit(corner, r, relay_send.at[3, s], sibling).start()

    def take_relayed(s):
        r = order(s)
        for owner in (me, across, along, corner):
            unit(owner + 1 - 2 * core, r, unit_send.at[0, s], me).wait_recv()

    def chunk(r, g):
        return ctx.at[r, pl.ds(g * pair, pair), :]

    def ctx_up(r, g):
        return remote(chunk(r, g), chunk(r, g), up_send.at[r, g], ctx_recv.at[r, g], (me, z + 1))

    def ctx_down(r, g):
        return remote(chunk(r, g), chunk(r, g), down_send.at[r, g], ctx_recv.at[r, g], (me, z - 1))

    inner = jnp.logical_and(z >= 1, z + 1 < n_head)

    def arrive(s, g):
        r = order(s)

        @pl.when(inner)
        def _():
            ctx_up(r, g).wait_recv()

        @pl.when(jnp.logical_and(inner, r < z))
        def _():
            ctx_up(r, g).start()

        @pl.when(jnp.logical_and(inner, r > z))
        def _():
            ctx_down(r, g).start()

    blocks = span // TILE + 1

    def attend(g):
        for dist in range(1, reach + 1):
            @pl.when(me >= dist)
            def _():
                halo(dist, g, 0, me).wait_recv()
                halo(dist, g, 1, me).wait_recv()
                if dist == 1:
                    @pl.when(even)
                    def _():
                        passed_on(g, 0).start()
                        passed_on(g, 1).start()

        @pl.loop(0, rows // TILE)
        def _(t):
            first = pl.multiple_of(t * TILE, TILE)
            q = jnp.concatenate([q_ref[g * groups + i, pl.ds(first, TILE), :] for i in range(groups)], 0)
            row = lax.broadcasted_iota(jnp.int32, (TILE, groups * TILE), 0)
            col = lax.rem(lax.broadcasted_iota(jnp.int32, (TILE, groups * TILE), 1), TILE)
            scores = []
            top = None
            for b in range(blocks):
                s = lax.dot_general(
                    k_ext[g, pl.ds(first + b * TILE, TILE), :], q,
                    (((1,), (1,)), ((), ())), preferred_element_type=jnp.float32,
                )
                valid = me * rows + first + b * TILE - span >= 0
                if b == 0:
                    s = jnp.where(jnp.logical_and(row > col, valid), s, MASKED)
                elif b == blocks - 1:
                    s = jnp.where(row <= col, s, MASKED)
                else:
                    s = jnp.where(valid, s, MASKED)
                scores.append(s)
                high = jnp.max(s, axis=0, keepdims=True)
                top = high if top is None else jnp.maximum(top, high)
            shift = top * (SCALE * LOG2E)
            total = None
            mixed = None
            for b in range(blocks):
                w = jnp.exp2(scores[b] * (SCALE * LOG2E) - shift)
                part_sum = jnp.sum(w, axis=0, keepdims=True)
                total = part_sum if total is None else total + part_sum
                o = jnp.dot(
                    v_ext[g, :, pl.ds(pl.multiple_of(first + b * TILE, TILE), TILE)], w.astype(jnp.bfloat16),
                    preferred_element_type=jnp.float32,
                )
                mixed = o if mixed is None else mixed + o
            result = (mixed / total).astype(jnp.bfloat16)
            for i in range(groups):
                ctx[z, pl.ds((g * groups + i) * size, size), pl.ds(first, TILE)] = result[:, i * TILE : (i + 1) * TILE]

        @pl.when(z + 1 < n_head)
        def _():
            ctx_up(z, g).start()

        @pl.when(z >= 1)
        def _():
            ctx_down(z, g).start()

    tile = next(t for t in range(feats, 0, -16) if feats % t == 0)

    def project(s, g, n=1):
        last = s == n_head - 1 and g + n == kv_heads
        r = order(s)
        if s > 0:
            @pl.when(jnp.logical_not(inner))
            def _():
                for i in range(n):
                    ctx_up(r, g + i).wait_recv()

        block = ctx[r, pl.ds(g * pair, n * pair), :]
        for j in range(sub):
            @pl.loop(0, feats // tile)
            def _(t):
                at = pl.ds(pl.multiple_of(t * tile, tile), tile)
                w = jnp.concatenate([w_all[g * groups + i, r, j, at, :] for i in range(n * groups)], 1)
                got = jnp.dot(w, block, preferred_element_type=jnp.float32)
                if s > 0 or g > 0:
                    got = got + acc[j, at, :]
                acc[j, at, :] = got
                if last:
                    squares[0] += jnp.sum((got * got).reshape(tile // 8, 8, rows), axis=0)

    loads = [pltpu.make_async_copy(src, dst, load_sem.at[i]) for i, (src, dst) in enumerate((
        (pos_hbm, pos_ref), (rate_hbm, rate_ref), (k_hbm, k_raw), (v_hbm, v_raw),
        (w_hbm, w_ref), (q_hbm, q_raw), (gain_hbm, gain_ref), (res_hbm, res_ref),
    ))]
    barrier = pltpu.get_barrier_semaphore()
    for d in range(1, n_seq):
        pl.semaphore_signal(barrier, inc=1, device_id=(lax.rem(me + d, n_seq), z), device_id_type=MESH)
    for d in range(1, n_head):
        pl.semaphore_signal(barrier, inc=1, device_id=(me, lax.rem(z + d, n_head)), device_id_type=MESH)
    for load in loads:
        load.start()

    def turned(x):
        x = jnp.swapaxes(x.astype(jnp.float32), 0, 1)
        return (x * cosine[None] + pltpu.roll(x, size // 2, 2) * sine[None]).astype(jnp.bfloat16)

    part = rows // 4
    for load in loads[:2]:
        load.wait()
    tokens = pos_ref[...].reshape(1, rows).astype(jnp.float32)
    early = lax.broadcasted_iota(jnp.int32, (size, size), 1) < size // 2
    for t in range(0, rows, size):
        angle = jnp.broadcast_to(tokens[:, t : t + size], (size, size)).T * rate_ref[...]
        cos_ref[t : t + size, :] = jnp.cos(angle)
        sine = jnp.sin(angle)
        sin_ref[t : t + size, :] = jnp.where(early, -sine, sine)
    loads[4].wait()
    pl.semaphore_wait(barrier, n_seq + n_head - 2)

    @pl.when(me // sub == z)
    def _():
        own_copy().start()

    @pl.when(me // sub != z)
    def _():
        own_climb().start()

    for word in LAUNCH:
        if word[0] != "H":
            scatter(others[int(word[1])])
    for load in loads[2:4]:
        load.wait()
    for t in range(0, rows, part):
        cosine, sine = cos_ref[t : t + part, :], sin_ref[t : t + part, :]
        k_ext[:, span + t : span + t + part, :] = turned(k_raw[t : t + part])
    for g in range(kv_heads):
        v_ext[g, :, span : span + rows] = v_raw[:, g, :].T
    for g in range(kv_heads):
        start_halo(g)
    squares[0] = jnp.zeros((8, rows), jnp.float32)
    loads[5].wait()
    for t in range(0, rows, part):
        cosine, sine = cos_ref[t : t + part, :], sin_ref[t : t + part, :]
        q_ref[:, t : t + part, :] = turned(q_raw[t : t + part])
    for dist in range(1, reach + 1):
        @pl.when(me < dist)
        def _():
            at = pl.ds(span - dist * rows, rows)
            k_ext[:, at, :] = jnp.zeros((kv_heads, rows, size), jnp.bfloat16)
            v_ext[:, :, at] = jnp.zeros((kv_heads, size, rows), jnp.bfloat16)
    loads[6].wait()
    gain_row = gain_ref[...].reshape(1, gain_ref.shape[0])
    for first in range(0, gain_ref.shape[0], LANES):
        count = min(LANES, gain_ref.shape[0] - first)
        gain_col[first : first + count, :] = jnp.broadcast_to(gain_row[:, first : first + count], (LANES, count)).T

    def take(n):
        take_piece(others[n])

    steps = {"T": take, "A": attend, "C": send_unit, "X": take_across, "Y": take_along, "D": take_corner,
             "S": take_relayed, "R": arrive, "P": project}
    for word in PLAN:
        steps[word[0]](*[int(c) for c in word[1:]])

    def sq(d, target):
        return remote(squares.at[0], squares.at[d], sq_send.at[d - 1], sq_recv.at[d - 1], (me, target))

    for d in range(1, n_head):
        sq(d, lax.rem(z + d, n_head)).start()
    for g in range(kv_heads):
        for dist in range(1, reach + 1):
            leaves = me + dist < n_seq
            if dist == 2:
                leaves = jnp.logical_and(even, leaves)

            @pl.when(leaves)
            def _():
                halo(dist, g, 0, me).wait_send()
                halo(dist, g, 1, me).wait_send()

        @pl.when(jnp.logical_and(even, me >= 1))
        def _():
            passed_on(g, 0).wait_send()
            passed_on(g, 1).wait_send()
    for target in others:
        piece(me, target, False).wait_send()
        source = target

        @pl.when(source // sub != z)
        def _():
            climb(source).wait_send()

    @pl.when(me // sub != z)
    def _():
        own_climb().wait_send()
    for s in range(n_head):
        for way in range(2):
            unit(me, s, unit_send.at[way, s], me).wait_send()
        unit(me, s, forward_send.at[s], me).wait_send()
        for way in range(4):
            unit(me, s, relay_send.at[way, s], me).wait_send()
    for g in range(kv_heads):
        for r in range(n_head):
            @pl.when(jnp.logical_and(r <= z, z + 1 < n_head))
            def _():
                ctx_up(r, g).wait_send()

            @pl.when(jnp.logical_and(r >= z, z >= 1))
            def _():
                ctx_down(r, g).wait_send()
    for d in range(1, n_head):
        sq(d, z).wait_recv()
    loads[7].wait()
    whole = jnp.sum(jnp.sum(squares[...], axis=0), axis=0, keepdims=True)
    inverse = lax.rsqrt(whole / (n_head * sub * feats) + EPS)
    for j in range(sub):
        at = pl.ds(j * feats, feats)
        gain = jnp.concatenate([gain_col[at, :]] * (rows // LANES), 1)
        out_ref[at, :] = (
            res_ref[at, :].astype(jnp.float32) + gain * (acc[j] * inverse)
        ).astype(jnp.bfloat16)

    for d in range(1, n_head):
        sq(d, z).wait_send()


def fits(rows, heads_rows, kv_heads, groups, feats, n_seq, n_head):
    return (
        n_seq == 8
        and n_head in (2, 4)
        and groups == 2
        and heads_rows == n_seq * LANES
        and rows % TILE == 0
        and VISIBLE_SPAN == 2 * rows
        and kv_heads * groups == n_seq
        and feats % 16 == 0
    )


def fused(positions, queries, keys, values, out_weight, post_gain, residual):
    n_seq, n_head = lax.axis_size("seq"), lax.axis_size("head")
    rows, kv_heads, size = keys.shape
    groups = queries.shape[1] // kv_heads
    feats = out_weight.shape[1]
    width = residual.shape[1]
    sub = n_seq // n_head
    reach = VISIBLE_SPAN // rows
    half = size // 2
    inverse = 10000.0 ** (-2.0 * jnp.arange(half, dtype=jnp.float32) / size)
    rate = jnp.concatenate([inverse, inverse])[None, :]
    bf16, f32 = jnp.bfloat16, jnp.float32
    dma = pltpu.SemaphoreType.DMA
    spec = pl.BlockSpec(memory_space=pltpu.VMEM)
    out = pl.pallas_call(
        functools.partial(layer_kernel, n_seq, n_head, kv_heads, groups, reach),
        out_shape=jax.ShapeDtypeStruct((width, rows), bf16),
        in_specs=[pl.BlockSpec(memory_space=pltpu.MemorySpace.HBM)] * 8,
        out_specs=spec,
        scratch_shapes=[
            pltpu.VMEM(queries.shape, bf16), pltpu.VMEM(keys.shape, bf16), pltpu.VMEM(keys.shape, bf16),
            pltpu.VMEM((rows,), jnp.int32), pltpu.VMEM((1, size), f32), pltpu.VMEM(out_weight.shape[::-1], bf16),
            pltpu.VMEM((width,), f32), pltpu.VMEM((width, rows), bf16), dma((8,)),
            pltpu.VMEM((rows, size), f32), pltpu.VMEM((rows, size), f32),
            pltpu.VMEM((kv_heads * groups, rows, size), bf16),
            pltpu.VMEM((width, LANES), f32),
            pltpu.VMEM((kv_heads, (reach + 1) * rows, size), bf16),
            pltpu.VMEM((kv_heads, size, (reach + 1) * rows), bf16),
            pltpu.VMEM((n_seq, feats, LANES), bf16),
            pltpu.VMEM((n_seq, n_head, sub, feats, LANES), bf16),
            pltpu.VMEM((n_head, kv_heads * groups * size, rows), bf16),
            pltpu.VMEM((sub, feats, rows), f32),
            pltpu.VMEM((n_head, 8, rows), f32),
            dma((reach, kv_heads, 2)), dma((reach, kv_heads, 2)), dma((kv_heads, 2)),
            dma((n_seq,)), dma((n_seq,)), dma, dma((n_seq,)), dma((n_head, sub)),
            dma((2, n_head)), dma((n_head,)), dma((4, n_head)), dma((n_seq, n_head)),
            dma((n_head, kv_heads)), dma((n_head, kv_heads)), dma((n_head, kv_heads)),
            dma((n_head,)), dma((n_head,)),
        ],
        compiler_params=pltpu.CompilerParams(has_side_effects=True, collective_id=0, vmem_limit_bytes=44 * 1024 * 1024),
    )(*[pltpu.with_memory_space_constraint(x, pltpu.MemorySpace.HBM) for x in (queries, keys, values, positions, rate, out_weight.T, post_gain, residual.T)])
    return out.T


def general(positions, queries, keys, values, out_weight, post_gain, residual):
    rows = queries.shape[0]
    kv_heads = keys.shape[1]
    query_groups = QUERY_HEADS // KEY_VALUE_HEADS
    q_rot = rotate(queries, positions)
    stacked = jnp.stack([rotate(keys, positions), values], 0)
    reach = (VISIBLE_SPAN + rows - 2) // rows
    pieces = []
    carried = stacked
    for hop in range(reach):
        carried = passed_along(carried, "seq", 1)
        pieces.insert(0, carried)
    extended = jnp.concatenate(pieces + [stacked], axis=1)
    extra = extended.shape[1] - rows
    anchor = lax.axis_index("seq") * rows
    tile_rows = q_rot.reshape(rows, kv_heads, query_groups, -1)
    scores = jnp.einsum("qhgd,khd->hgqk", tile_rows, extended[0], preferred_element_type=jnp.float32) * SCALE
    query_index = anchor + jnp.arange(rows, dtype=jnp.int32)
    key_index = anchor - extra + jnp.arange(extra + rows, dtype=jnp.int32)
    gap = query_index[:, None] - key_index[None, :]
    allowed = (gap >= 0) & (gap < VISIBLE_SPAN) & (key_index[None, :] >= 0)
    scores = jnp.where(allowed, scores, MASKED)
    top = jnp.max(scores, axis=-1, keepdims=True)
    weights = jnp.exp(scores - top)
    probs = (weights / jnp.sum(weights, axis=-1, keepdims=True)).astype(jnp.bfloat16)
    context = jnp.einsum("hgqk,khd->qhgd", probs, extended[1], preferred_element_type=jnp.float32)
    context = context.astype(jnp.bfloat16).reshape(rows, -1)
    partial_value = jnp.dot(
        context,
        lax.all_gather(out_weight, "seq", axis=1, tiled=True),
        preferred_element_type=jnp.float32,
    )
    attended = lax.psum_scatter(
        partial_value.astype(jnp.bfloat16), "head", scatter_dimension=1, tiled=True
    ).astype(jnp.float32)
    squares = lax.psum(jnp.sum(attended * attended, axis=1), "head")
    scaled = attended * lax.rsqrt(squares / D + EPS)[:, None]
    result = residual.astype(jnp.float32) + post_gain[None, :] * scaled
    return result.astype(jnp.bfloat16)


def on_device(positions, queries, keys, values, out_weight, post_gain, residual):
    n_seq, n_head = lax.axis_size("seq"), lax.axis_size("head")
    rows, kv_heads, _ = keys.shape
    body = fused if fits(rows, out_weight.shape[0], kv_heads, queries.shape[1] // kv_heads, out_weight.shape[1], n_seq, n_head) else general
    return body(positions, queries, keys, values, out_weight, post_gain, residual)


def solution(mesh):
    return jax.shard_map(
        on_device,
        mesh=mesh,
        in_specs=(
            P("seq"),
            P("seq", "head", None),
            P("seq", "head", None),
            P("seq", "head", None),
            P("head", "seq"),
            P("head"),
            P("seq", "head"),
        ),
        out_specs=P("seq", "head"),
        check_vma=False,
    )
```
